32 devices in a mesh: grp: 4 (over x, core), blk: 2 (over y), set: 4 (over z).
Axes of the slice: x: 2, y: 2, z: 4, core: 2. Of those that a mesh axis runs over, the one named last changes fastest.
Arguments:
- queries: bfloat16 [4096, 384], P(('grp', 'blk', 'set')), may hold values from -8 to 8
- keys: bfloat16 [4096, 384], P(('grp', 'blk', 'set')), may hold values from -8 to 8
- values: bfloat16 [4096, 384], P(('grp', 'blk', 'set')), may hold values from -6 to 6
- valid: int32 [4096], P(('grp', 'blk', 'set')), may hold values 0 or 1
- offsets: int32 [2, 6], replicated, may hold values from 0 to 7, as said below
- w_out: bfloat16 [384, 768], replicated, may hold values from -0.3125 to 0.3125
Outputs:
- projected: bfloat16 [4096, 768], P(('grp', 'blk', 'set'))
The draws below stay inside these ranges and needn't reach their ends.
Inputs may be any that keep to these rules, and one draw needn't show every extreme that they name: offsets[0, h] lies in 0 to 1 and offsets[1, h] - offsets[0, h] is a multiple of 2 for every head h.
All inputs are finite; a program needn't handle non-finite values. No bound on the sum of `valid` on one device may be relied on, other than what follows from the above.
Results may differ from the reference program's by a relative error of at most 0.0015.
The reference program's roundings to bfloat16 on the way count: a program that leaves them out, or rounds other values in their place, can miss the bound.
Values may be sent and summed in bfloat16 or wider, within the bound.
A program may use at most 64 MiB of HBM per device.

```python
import math
import jax
import jax.numpy as jnp
from jax import lax

MODEL_WIDTH = 768
HEAD_COUNT = 6
HD = 64
ATT_WIDTH = 384
FIRST_SEGMENT = 512
TOKENS = 4096
SECOND_DILATION = 2
THIRD_DILATION = 8


def drawn_pair(key):
    base_key = jax.random.fold_in(key, 17)
    first_key, second_key = jax.random.split(base_key, 2)
    full_shape = (TOKENS, ATT_WIDTH)
    query_draw = jnp.clip(1.5 * jax.random.normal(first_key, full_shape, jnp.float32), -8.0, 8.0)
    key_draw = jnp.clip(1.5 * jax.random.normal(second_key, full_shape, jnp.float32), -8.0, 8.0)
    return (query_draw, key_draw)


def draw_queries(key, part):
    return drawn_pair(key)[0].astype(jnp.bfloat16)


def draw_keys(key, part):
    return drawn_pair(key)[1].astype(jnp.bfloat16)


def draw_offsets(key, part):
    base_key = jax.random.fold_in(key, 29)
    bottom_key, ceiling_key = jax.random.split(base_key)
    middle_shift = jax.random.randint(bottom_key, (HEAD_COUNT,), 0, SECOND_DILATION)
    outer_shift = middle_shift + SECOND_DILATION * jax.random.randint(ceiling_key, (HEAD_COUNT,), 0, THIRD_DILATION // SECOND_DILATION)
    return jnp.stack([middle_shift, outer_shift]).astype(jnp.int32)


def set_ends(drawn, own_key, low, high):
    longest = drawn.shape.index(max(drawn.shape))
    spots = []
    for shift in (0, 1):
        where = [jax.random.randint(jax.random.fold_in(own_key, axis), (), 0, length) for axis, length in enumerate(drawn.shape)]
        where[longest] = (where[longest] + shift) % drawn.shape[longest]
        spots.append(tuple(where))
    return drawn.at[spots[0]].set(low).at[spots[1]].set(high)


def level_of(key, shape, cuts, least, largest):
    def one(dim, parts):
        steps = jax.random.uniform(jax.random.fold_in(jax.random.fold_in(key, 6), dim), (parts,), jnp.float32, least / len(cuts), largest / len(cuts))
        return jnp.repeat(jnp.exp(steps), shape[dim] // parts).reshape((-1,) + (1,) * (len(shape) - dim - 1))

    loudness = one(*cuts[0])
    for cut in cuts[1:]:
        loudness = loudness * one(*cut)
    return loudness


def normal_values(own_key, extent, width, limit, cuts=(), kind=jnp.bfloat16):
    array = jax.random.normal(own_key, extent, jnp.float32) * width
    if len(cuts) > 0:
        array = level_of(own_key, extent, cuts, -0.22, 0.18) * array
    return jnp.clip(array, min=-limit, max=limit).astype(kind)


def setup_inputs(seed: int = 0) -> dict:
    streams_of = jax.random.split(jax.random.key(seed), 7)
    return {
        "queries": draw_queries(jax.random.fold_in(streams_of[6], 71), 0),
        "keys": draw_keys(jax.random.fold_in(streams_of[6], 71), 0),
        "values": normal_values(streams_of[2], (TOKENS, ATT_WIDTH), 1.0, 6.0, ((0, 32),)),
        "valid": set_ends((jax.random.randint(streams_of[3], (TOKENS,), 0, 4) < 3).astype(jnp.int32), jax.random.fold_in(streams_of[3], 1), 0, 1),
        "offsets": draw_offsets(jax.random.fold_in(streams_of[6], 71), 0),
        "w_out": normal_values(streams_of[5], (ATT_WIDTH, MODEL_WIDTH), ATT_WIDTH ** -0.5, 0.3125),
    }


def head_attend(query_head, key_head, value_head, key_allowed, self_slot, scaling):
    scores = lax.dot_general(query_head, key_head, (((1,), (1,)), ((), ())), preferred_element_type=jnp.float32) * scaling
    columns = jnp.arange(key_head.shape[0], dtype=jnp.int32)
    allowed = key_allowed[None, :] | (columns[None, :] == self_slot[:, None])
    scores = jnp.where(allowed, scores, jnp.float32(-1e+30))
    highest = lax.optimization_barrier(jnp.max(scores, axis=1, keepdims=True))
    weights = jnp.exp(scores - highest)
    totals = lax.optimization_barrier(jnp.sum(weights, axis=1))
    mixture = jnp.dot(weights.astype(jnp.bfloat16), value_head, preferred_element_type=jnp.float32) / totals[:, None]
    return (mixture, highest[:, 0] + jnp.log(totals))

def attend(queries, keys, values, key_allowed, self_slot):
    row_count = queries.shape[0]
    length = keys.shape[0]
    heads_query = queries.reshape(row_count, HEAD_COUNT, HD).transpose(1, 0, 2)
    heads_key = keys.reshape(length, HEAD_COUNT, HD).transpose(1, 0, 2)
    heads_value = values.reshape(length, HEAD_COUNT, HD).transpose(1, 0, 2)
    scaling = 1.0 / math.sqrt(HD)
    mixture, log_totals = lax.map(lambda packed: head_attend(packed[0], packed[1], packed[2], packed[3], self_slot, scaling), (heads_query, heads_key, heads_value, key_allowed.T))
    return (mixture.transpose(1, 0, 2).reshape(row_count, HEAD_COUNT * HD), log_totals.T)

def selector_table(shift_amount, cycle_length):
    return jnp.arange(cycle_length, dtype=jnp.int32)[:, None] == shift_amount[None, :]

def pick_rows(matrix, shift_amount, cycle_length):
    row_total = matrix.shape[0]
    selector = selector_table(shift_amount, cycle_length)
    blocks = matrix.reshape(row_total // cycle_length, cycle_length, HEAD_COUNT, HD)
    chosen = lax.optimization_barrier(jnp.sum(jnp.where(selector[None, :, :, None], blocks, jnp.zeros((), matrix.dtype)), axis=1))
    return chosen.reshape(row_total // cycle_length, HEAD_COUNT * HD)

def pick_flags(key_flags, shift_amount, cycle_length):
    row_total = key_flags.shape[0]
    selector = selector_table(shift_amount, cycle_length)
    blocks = key_flags.reshape(row_total // cycle_length, cycle_length)
    return lax.optimization_barrier(jnp.sum(jnp.where(selector[None, :, :], blocks[:, :, None], jnp.zeros((), key_flags.dtype)), axis=1))

def spread_back(mixture, log_totals, shift_amount, cycle_length):
    row_count = mixture.shape[0]
    selector = selector_table(shift_amount, cycle_length)
    wide = jnp.where(selector[None, :, :, None], mixture.reshape(row_count, 1, HEAD_COUNT, HD), jnp.float32(0.0))
    spread_totals = jnp.where(selector[None, :, :], log_totals[:, None, :], jnp.float32(0.0))
    present = jnp.broadcast_to(selector[None, :, :], (row_count, cycle_length, HEAD_COUNT))
    return (wide.reshape(row_count * cycle_length, HEAD_COUNT * HD), spread_totals.reshape(row_count * cycle_length, HEAD_COUNT), present.reshape(row_count * cycle_length, HEAD_COUNT))

def combine(levels):
    highest = levels[0][1]
    for entry in levels[1:]:
        highest = jnp.maximum(highest, jnp.where(entry[2], entry[1], highest))
    numerator = jnp.zeros(levels[0][0].shape, jnp.float32)
    denominator = jnp.zeros(levels[0][1].shape, jnp.float32)
    for entry in levels:
        scaled = jnp.where(entry[2], jnp.exp(entry[1] - highest), jnp.float32(0.0))
        expanded = jnp.broadcast_to(scaled[:, :, None], (scaled.shape[0], HEAD_COUNT, HD)).reshape(scaled.shape[0], HEAD_COUNT * HD)
        numerator = numerator + entry[0] * expanded
        denominator = denominator + scaled
    wide_denominator = jnp.broadcast_to(denominator[:, :, None], (denominator.shape[0], HEAD_COUNT, HD)).reshape(denominator.shape[0], HEAD_COUNT * HD)
    return numerator / wide_denominator

def segmented(queries, keys, values, key_allowed, segment):
    total_rows = queries.shape[0]
    pieces = total_rows // segment
    slot_index = jnp.arange(segment, dtype=jnp.int32)
    mixture, log_totals = lax.map(lambda packed: attend(packed[0], packed[1], packed[2], packed[3], slot_index), (queries.reshape(pieces, segment, HEAD_COUNT * HD), keys.reshape(pieces, segment, HEAD_COUNT * HD), values.reshape(pieces, segment, HEAD_COUNT * HD), key_allowed.reshape(pieces, segment, HEAD_COUNT)))
    return (mixture.reshape(total_rows, HEAD_COUNT * HD), log_totals.reshape(total_rows, HEAD_COUNT))

def reference(queries, keys, values, valid, offsets, w_out):
    total_rows = queries.shape[0]
    key_flags = valid.astype(jnp.float32)
    dense_allowed = jnp.broadcast_to((valid == 1)[:, None], (total_rows, HEAD_COUNT))
    dense_level = segmented(queries, keys, values, dense_allowed, FIRST_SEGMENT)
    levels = [(dense_level[0], dense_level[1], jnp.ones((total_rows, HEAD_COUNT), jnp.bool_))]
    for shift_amount, cycle_length in ((offsets[0], SECOND_DILATION), (offsets[1], THIRD_DILATION)):
        sparse_query = pick_rows(queries, shift_amount, cycle_length)
        sparse_key = pick_rows(keys, shift_amount, cycle_length)
        sparse_value = pick_rows(values, shift_amount, cycle_length)
        sparse_allowed = pick_flags(key_flags, shift_amount, cycle_length) > 0.5
        mixture, log_totals = segmented(sparse_query, sparse_key, sparse_value, sparse_allowed, FIRST_SEGMENT)
        levels.append(spread_back(mixture, log_totals, shift_amount, cycle_length))
    attention = combine(levels).astype(jnp.bfloat16)
    return jnp.dot(attention, w_out, preferred_element_type=jnp.float32).astype(jnp.bfloat16)
```

```python
import functools

import jax
import jax.numpy as jnp
from jax import lax
from jax.experimental import pallas as pl
from jax.experimental.pallas import tpu as pltpu
from jax.sharding import PartitionSpec as P

HEAD_COUNT = 6
HD = 64
LANES = 128
UNIT = 16
FLAG_STRIDE = 8
CHUNKS = HEAD_COUNT * HD // LANES
SETS = ((0, 3, 4), (2, 1, 5))
PARTS = 3
MESH = pl.DeviceIdType.MESH
NEG = -1e30


def units(count):
    return -(-count // UNIT)


def split_pow2(x, size):
    shift = size.bit_length() - 1
    return lax.shift_right_logical(x, shift), x & (size - 1)


class Plan:
    def __init__(self, grp, blk, n, rows):
        self.grp, self.blk, self.n, self.rows = grp, blk, n, rows
        self.period = grp * blk
        self.c3 = rows // self.period
        c2 = rows // blk
        self.counts = (self.c3, c2 - self.c3, rows - c2)
        self.units = tuple(units(c) for c in self.counts)
        self.sizes = tuple(u * UNIT for u in self.units)
        self.starts = (0, self.sizes[0], self.sizes[0] + self.sizes[1])
        self.total = sum(self.sizes)

    def source(self, t):
        a = t
        b = t - self.starts[1]
        c = t - self.starts[2]
        bv, bg = split_pow2(b, self.c3)
        cv, cg = split_pow2(c, self.c3)
        ck, cm = split_pow2(cv, self.grp)
        is_a = t < self.starts[1]
        is_b = t < self.starts[2]
        group = jnp.where(is_a, a, jnp.where(is_b, bg, cg))
        slot = jnp.where(is_a, 0, jnp.where(is_b, (bv + 1) * self.blk, cm * self.blk + ck + 1))
        local = jnp.where(is_a, a, jnp.where(is_b, b, c))
        count = jnp.where(is_a, self.counts[0], jnp.where(is_b, self.counts[1], self.counts[2]))
        return jnp.where(local < count, group * self.period, -(1 << 20)), slot


def flip(s, r):
    step = 1
    while step <= r:
        if r & step:
            s = s + step * (1 - 2 * ((s // step) % 2))
        step *= 2
    return s


def kernel(
    plan, q_hbm, k_hbm, v_hbm, valid_hbm, offs_hbm, w_hbm, o_ref,
    q_ref, k_ref, v_ref, valid_ref, offs_ref, w_ref,
    buf_a, buf_b, buf_c, snd_a, snd_b, snd_c, snd_q, qbuf, ret_s, ret_r, own_o, back_hot,
    load, zsend, zrecv, qsend, qrecv, asend, arecv, bsend, brecv, fsend, frecv, rsend, rrecv,
):
    G, B, N = plan.grp, plan.blk, plan.n
    R = plan.total
    K = G // 2
    gi, bi, si = lax.axis_index("grp"), lax.axis_index("blk"), lax.axis_index("set")
    core = gi % 2
    partner = gi + 1 - 2 * core
    even = si % 2 == 0

    def peer(sx, sy):
        return (lax.rem(gi + 2 * sx, G), lax.rem(bi + sy, B), si)

    across = [(sx, sy) for sx in range(K) for sy in range(B) if sx or sy]

    barrier = pltpu.get_barrier_semaphore()

    def greet(device):
        pl.semaphore_signal(barrier, inc=1, device_id=device, device_id_type=MESH)

    for r in range(N - 1, 0, -1):
        greet((gi, bi, flip(si, r)))
    for sx, sy in across:
        greet(peer(sx, sy))
    greet((partner, bi, si))

    loads = [
        pltpu.make_async_copy(src, dst, load.at[i])
        for i, (src, dst) in enumerate(
            [
                (offs_hbm, offs_ref), (valid_hbm, valid_ref), (k_hbm, k_ref),
                (v_hbm, v_ref), (q_hbm, q_ref), (w_hbm, w_ref),
            ]
        )
    ]
    for copy in loads:
        copy.start()
    for copy in loads[:5]:
        copy.wait()

    lane = lax.broadcasted_iota(jnp.int32, (R, LANES), 1)
    left = lane < HD
    base, slot = plan.source(lax.broadcasted_iota(jnp.int32, (R, plan.rows), 0))
    token = lax.broadcasted_iota(jnp.int32, (R, plan.rows), 1)
    valid_row = (valid_ref[...] > 0).astype(jnp.float32)
    flag_lane = lax.broadcasted_iota(jnp.int32, (UNIT, LANES), 1)

    moved = {}
    columns = {}
    for h in range(HEAD_COUNT):
        cols = slice((h // 2) * LANES, (h // 2 + 1) * LANES)
        packed = jnp.concatenate([q_ref[:, cols], k_ref[:, cols], v_ref[:, cols]], axis=1)
        hit = token == base + ((slot + offs_ref[1, h]) & (plan.period - 1))
        onehot = jnp.where(hit, jnp.float32(1), jnp.float32(0))
        moved[h] = jnp.dot(onehot.astype(jnp.bfloat16), packed, preferred_element_type=jnp.float32)
        columns[h] = jnp.sum(onehot * valid_row, axis=1, keepdims=True)

    def piece(h, which):
        return moved[h][:, which * LANES:(which + 1) * LANES]

    packs = []
    for number, (a, b, c) in enumerate(SETS):
        flags = jnp.zeros((UNIT, LANES), jnp.float32)
        for j, h in enumerate((a, b, c)):
            for u in range(R // UNIT):
                flags = jnp.where(
                    flag_lane == u * FLAG_STRIDE + j, columns[h][u * UNIT:(u + 1) * UNIT, :], flags
                )
        turned = pltpu.roll(piece(c, 2), HD, 1)
        mixed = jnp.where(left, piece(c, 1), turned) if number == 0 else jnp.where(left, turned, piece(c, 1))
        packs.append(
            (
                jnp.where(left, piece(a, 1), piece(b, 1)),
                jnp.where(left, piece(a, 2), piece(b, 2)),
                mixed,
                jnp.where(left, piece(a, 0), piece(b, 0)) * 0.125,
                piece(c, 0) * 0.125,
                flags,
            )
        )
    mine = [jnp.where(even, x, y).astype(jnp.bfloat16) for x, y in zip(*packs)]
    other = [jnp.where(even, y, x).astype(jnp.bfloat16) for x, y in zip(*packs)]
    a_end, b_end = plan.starts[1], plan.starts[2]
    for j in range(PARTS):
        buf_a[0, 0, 0, j] = mine[j][:a_end]
        snd_a[j] = other[j][:a_end]
        buf_b[0, 0, j] = mine[j][a_end:b_end]
        snd_b[j] = other[j][a_end:b_end]
        buf_c[0, j] = mine[j][b_end:]
        snd_c[j] = other[j][b_end:]
    buf_a[0, 0, 0, PARTS, 0:UNIT] = mine[5]
    snd_a[PARTS, 0:UNIT] = other[5]
    for j in range(2):
        qbuf[0, j] = mine[3 + j]
        snd_q[j] = other[3 + j]

    pl.semaphore_wait(barrier, (N - 1) + len(across) + 1)

    def zcopy(part, r):
        own = (buf_a.at[0, 0, 0], buf_b.at[0, 0], buf_c.at[0])[part]
        sent = (snd_a, snd_b, snd_c)[part]
        return pltpu.make_async_remote_copy(
            src_ref=sent if r % 2 else own,
            dst_ref=(buf_a.at[0, 0, r], buf_b.at[0, r], buf_c.at[r])[part],
            send_sem=zsend.at[part, r], recv_sem=zrecv.at[part, r],
            device_id=(gi, bi, flip(si, r)), device_id_type=MESH,
        )

    def qcopy():
        return pltpu.make_async_remote_copy(
            src_ref=snd_q, dst_ref=qbuf.at[1], send_sem=qsend, recv_sem=qrecv,
            device_id=(gi, bi, flip(si, 1)), device_id_type=MESH,
        )

    def acopy(sx, sy, r):
        tx, ty = 2 * ((K - sx) % K), (B - sy) % B
        return pltpu.make_async_remote_copy(
            src_ref=buf_a.at[0, 0, r], dst_ref=buf_a.at[tx, ty, r],
            send_sem=asend.at[sx, sy, r], recv_sem=arecv.at[tx // 2, ty, r],
            device_id=peer(sx, sy), device_id_type=MESH,
        )

    def bcopy(sy, r):
        return pltpu.make_async_remote_copy(
            src_ref=buf_b.at[0, r], dst_ref=buf_b.at[B - sy, r],
            send_sem=bsend.at[sy, r], recv_sem=brecv.at[B - sy, r],
            device_id=peer(0, sy), device_id_type=MESH,
        )

    def fcopy(x, y):
        return pltpu.make_async_remote_copy(
            src_ref=buf_a.at[2 * x, y], dst_ref=buf_a.at[2 * x + 1, y],
            send_sem=fsend.at[x, y], recv_sem=frecv.at[x, y],
            device_id=(partner, bi, si), device_id_type=MESH,
        )

    def rcopy(j):
        return pltpu.make_async_remote_copy(
            src_ref=ret_s.at[j], dst_ref=ret_r.at[j], send_sem=rsend.at[j], recv_sem=rrecv.at[j],
            device_id=(gi, bi, flip(si, 1)), device_id_type=MESH,
        )

    def spread_a(r):
        for sx, sy in across:
            acopy(sx, sy, r).start()

    def spread_b(r):
        for sy in range(1, B):
            bcopy(sy, r).start()

    order = list(range(N - 1, 0, -1))
    for r in order:
        zcopy(0, r).start()
    spread_a(0)
    for r in order:
        zcopy(1, r).start()
    spread_b(0)
    for r in order[:-1]:
        zcopy(2, r).start()
    if N > 1:
        qcopy().start()
        zcopy(2, 1).start()

    token = lax.broadcasted_iota(jnp.int32, (plan.rows, R), 0)
    base, slot = plan.source(lax.broadcasted_iota(jnp.int32, (plan.rows, R), 1))
    for h in range(HEAD_COUNT):
        hit = token == base + ((slot + offs_ref[1, h]) & (plan.period - 1))
        back_hot[h] = jnp.where(hit, jnp.float32(1), jnp.float32(0)).astype(jnp.bfloat16)

    for r in range(1, N):
        zcopy(0, r).wait_recv()
        spread_a(r)
    fcopy(0, 0).start()
    for r in range(1, N):
        zcopy(1, r).wait_recv()
        spread_b(r)
    for sx, sy in across:
        for r in range(N):
            acopy((K - sx) % K, (B - sy) % B, r).wait_recv()
        fcopy(sx, sy).start()

    head_pick = lax.broadcasted_iota(jnp.int32, (FLAG_STRIDE, LANES), 1) & (FLAG_STRIDE - 1)
    head_pick = head_pick == lax.broadcasted_iota(jnp.int32, (FLAG_STRIDE, LANES), 0)
    head_pick = jnp.where(head_pick, jnp.float32(1), jnp.float32(0)).astype(jnp.bfloat16)

    def gather(level, at):
        pieces = []
        for u in range(plan.units[0]):
            rows = slice(u * UNIT, (u + 1) * UNIT)
            part = (buf_a[0, 0, :, at, rows], buf_a[0, :, :, at, rows], buf_a[:, :, :, at, rows])[level]
            pieces.append(part.reshape(-1, LANES))
        if level < 2:
            for u in range(plan.units[1]):
                rows = slice(u * UNIT, (u + 1) * UNIT)
                part = buf_b[0, :, at, rows] if level == 0 else buf_b[:, :, at, rows]
                pieces.append(part.reshape(-1, LANES))
        if level == 0:
            for u in range(plan.units[2]):
                pieces.append(buf_c[:, at, u * UNIT:(u + 1) * UNIT].reshape(-1, LANES))
        return pieces[0] if len(pieces) == 1 else jnp.concatenate(pieces, axis=0)

    def level_attend(level):
        M = (R, b_end, a_end)[level]
        tiles = M // UNIT
        devices = (N, B * N, G * B * N)[level]
        per_unit = devices * UNIT
        rows = slice(0, UNIT)
        at = PARTS
        tall = (buf_a[0, 0, :, at, rows], buf_a[0, :, :, at, rows], buf_a[:, :, :, at, rows])[level]
        tall = tall.reshape(per_unit, LANES).astype(jnp.float32)
        unit_lane = lax.broadcasted_iota(jnp.int32, (per_unit, LANES), 1) // FLAG_STRIDE
        tall = [jnp.where(unit_lane == u, tall, 0.0).astype(jnp.bfloat16) for u in range(tiles)]
        tall = tall[0] if tiles == 1 else jnp.concatenate(tall, axis=0)
        ok = lax.dot_general(
            head_pick, tall, (((1,), (1,)), ((), ())), preferred_element_type=jnp.float32
        )
        keys = per_unit * tiles
        t = lax.broadcasted_iota(jnp.int32, (M, keys), 0)
        spot = lax.broadcasted_iota(jnp.int32, (M, keys), 1) - ((t // UNIT) * per_unit + (t % UNIT))
        half_lane = lax.broadcasted_iota(jnp.int32, (M, LANES), 1) < HD
        value_lane = half_lane != even

        def softmax(scores, j, who):
            s = jnp.where((spot == who * UNIT) | (ok[j:j + 1, :] > 0.5), scores, NEG)
            top = jnp.max(s, axis=1, keepdims=True)
            weight = jnp.exp(s - top)
            return weight.astype(jnp.bfloat16), top, jnp.sum(weight, axis=1, keepdims=True)

        contract = (((1,), (1,)), ((), ()))
        pair_k, pair_v, single = gather(level, 0), gather(level, 1), gather(level, 2)
        zero = jnp.zeros((M, LANES), jnp.bfloat16)
        results = [[None, None], [None, None]]
        for who in (1, 0):
            q = qbuf[who, 0, 0:M]
            both = jnp.concatenate([jnp.where(half_lane, q, zero), jnp.where(half_lane, zero, q)], axis=0)
            scores = lax.dot_general(both, pair_k, contract, preferred_element_type=jnp.float32)
            weights = [softmax(scores[j * M:(j + 1) * M], j, who) for j in range(2)]
            mixed = jnp.dot(
                jnp.concatenate([w[0] for w in weights], axis=0), pair_v, preferred_element_type=jnp.float32
            )
            results[who][0] = (
                jnp.where(half_lane, mixed[:M] / weights[0][2], mixed[M:] / weights[1][2]),
                jnp.where(
                    half_lane,
                    weights[0][1] + jnp.log(weights[0][2]),
                    weights[1][1] + jnp.log(weights[1][2]),
                ),
            )
        for who in (1, 0):
            q = jnp.where(value_lane, zero, qbuf[who, 1, 0:M])
            scores = lax.dot_general(q, single, contract, preferred_element_type=jnp.float32)
            weight, top, total = softmax(scores, 2, who)
            mixed = jnp.dot(weight, single, preferred_element_type=jnp.float32)
            results[who][1] = (mixed / total, jnp.broadcast_to(top + jnp.log(total), (M, LANES)))
        return results

    if N > 1:
        qcopy().wait_recv()
    for r in range(1, N):
        zcopy(2, r).wait_recv()
    first = level_attend(0)
    for x in range(K):
        for y in range(B):
            fcopy(x, y).wait_recv()
    third = level_attend(2)
    for sy in range(1, B):
        for r in range(N):
            bcopy(B - sy, r).wait_recv()
    second = level_attend(1)

    def combine(levels):
        top = functools.reduce(jnp.maximum, [lse for _, lse in levels])
        shares = [jnp.exp(lse - top) for _, lse in levels]
        return sum(s * o for s, (o, _) in zip(shares, levels)) / sum(shares)

    for who in (1, 0):
        for j in range(2):
            (o1, l1), (o2, l2), (o3, l3) = first[who][j], second[who][j], third[who][j]
            mixed = jnp.concatenate(
                [
                    combine([(o1[:a_end], l1[:a_end]), (o2[:a_end], l2[:a_end]), (o3, l3)]),
                    combine([(o1[a_end:b_end], l1[a_end:b_end]), (o2[a_end:], l2[a_end:])]),
                    o1[b_end:],
                ],
                axis=0,
            ).astype(jnp.bfloat16)
            if who == 1:
                ret_s[j] = mixed
                rcopy(j).start()
            else:
                own_o[j] = mixed
    loads[5].wait()
    for j in range(2):
        rcopy(j).wait_recv()

    sets = [
        (jnp.where(even, own_o[j], ret_r[j]), jnp.where(even, ret_r[j], own_o[j])) for j in range(2)
    ]
    (zero_pair, one_pair), (zero_single, one_single) = sets
    singles = jnp.where(left, one_single, zero_single)
    out_left = lax.broadcasted_iota(jnp.int32, (plan.rows, LANES), 1) < HD
    attention, weights = [], []
    for value, (a, b) in ((zero_pair, SETS[0][:2]), (one_pair, SETS[1][:2]), (singles, (SETS[1][2], SETS[0][2]))):
        back = [jnp.dot(back_hot[h], value, preferred_element_type=jnp.float32) for h in (a, b)]
        attention.append(jnp.where(out_left, back[0], back[1]).astype(jnp.bfloat16))
        weights += [w_ref[a * HD:(a + 1) * HD, :], w_ref[b * HD:(b + 1) * HD, :]]
    attention = jnp.concatenate(attention, axis=1)
    weights = jnp.concatenate(weights, axis=0)
    o_ref[...] = jnp.dot(attention, weights, preferred_element_type=jnp.float32).astype(o_ref.dtype)

    for r in range(1, N):
        for part in range(3):
            zcopy(part, r).wait_send()
    if N > 1:
        qcopy().wait_send()
    for r in range(N):
        for sx, sy in across:
            acopy(sx, sy, r).wait_send()
        for sy in range(1, B):
            bcopy(sy, r).wait_send()
    for x in range(K):
        for y in range(B):
            fcopy(x, y).wait_send()
    for j in range(2):
        rcopy(j).wait_send()


def solution(mesh):
    G, B, N = mesh.shape["grp"], mesh.shape["blk"], mesh.shape["set"]

    def per_device(queries, keys, values, valid, offsets, w_out):
        rows, width = queries.shape
        plan = Plan(G, B, N, rows)
        vmem = pl.BlockSpec(memory_space=pltpu.VMEM)
        anywhere = pl.BlockSpec(memory_space=pl.ANY)
        dma = pltpu.SemaphoreType.DMA
        ra, rb, rc = plan.sizes
        R = plan.total
        bf16 = jnp.bfloat16
        return pl.pallas_call(
            functools.partial(kernel, plan),
            out_shape=jax.ShapeDtypeStruct((rows, w_out.shape[1]), bf16),
            in_specs=[anywhere] * 6,
            out_specs=vmem,
            scratch_shapes=[
                pltpu.VMEM((rows, width), bf16),
                pltpu.VMEM((rows, width), bf16),
                pltpu.VMEM((rows, width), bf16),
                pltpu.VMEM((1, rows), jnp.int32),
                pltpu.SMEM(offsets.shape, jnp.int32),
                pltpu.VMEM(w_out.shape, bf16),
                pltpu.VMEM((G, B, N, PARTS + 1, ra, LANES), bf16),
                pltpu.VMEM((B, N, PARTS, rb, LANES), bf16),
                pltpu.VMEM((N, PARTS, rc, LANES), bf16),
                pltpu.VMEM((PARTS + 1, ra, LANES), bf16),
                pltpu.VMEM((PARTS, rb, LANES), bf16),
                pltpu.VMEM((PARTS, rc, LANES), bf16),
                pltpu.VMEM((2, R, LANES), bf16),
                pltpu.VMEM((2, 2, R, LANES), bf16),
                pltpu.VMEM((2, R, LANES), bf16),
                pltpu.VMEM((2, R, LANES), bf16),
                pltpu.VMEM((2, R, LANES), bf16),
                pltpu.VMEM((HEAD_COUNT, rows, R), bf16),
                dma((6,)),
                dma((3, N)),
                dma((3, N)),
                dma,
                dma,
                dma((G // 2, B, N)),
                dma((G // 2, B, N)),
                dma((B, N)),
                dma((B, N)),
                dma((G // 2, B)),
                dma((G // 2, B)),
                dma((2,)),
                dma((2,)),
            ],
            compiler_params=pltpu.CompilerParams(
                collective_id=0, has_side_effects=True, vmem_limit_bytes=60 * 1024 * 1024
            ),
        )(queries, keys, values, valid.reshape(1, rows), offsets, w_out)

    rows_spec = P(("grp", "blk", "set"), None)
    return jax.shard_map(
        per_device,
        mesh=mesh,
        in_specs=(rows_spec, rows_spec, rows_spec, P(("grp", "blk", "set")), P(), P()),
        out_specs=rows_spec,
        check_vma=False,
    )
```

```python
import functools

import jax
import jax.numpy as jnp
from jax import lax
from jax.experimental import pallas as pl
from jax.experimental.pallas import tpu as pltpu
from jax.sharding import PartitionSpec as P

HEAD_COUNT = 6
HD = 64
LANES = 128
UNIT = 16
FLAG_STRIDE = 8
CHUNKS = HEAD_COUNT * HD // LANES
SETS = ((0, 3, 4), (2, 1, 5))
PARTS = 3
MESH = pl.DeviceIdType.MESH
NEG = -1e30


def units(count):
    return -(-count // UNIT)


def split_pow2(x, size):
    shift = size.bit_length() - 1
    return lax.shift_right_logical(x, shift), x & (size - 1)


class Plan:
    def __init__(self, grp, blk, n, rows):
        self.grp, self.blk, self.n, self.rows = grp, blk, n, rows
        self.period = grp * blk
        self.c3 = rows // self.period
        c2 = rows // blk
        self.counts = (self.c3, c2 - self.c3, rows - c2)
        self.units = tuple(units(c) for c in self.counts)
        self.sizes = tuple(u * UNIT for u in self.units)
        self.starts = (0, self.sizes[0], self.sizes[0] + self.sizes[1])
        self.total = sum(self.sizes)
        self.half = units(-(-self.total // 2)) * UNIT

    def source(self, t):
        a = t
        b = t - self.starts[1]
        c = t - self.starts[2]
        bv, bg = split_pow2(b, self.c3)
        cv, cg = split_pow2(c, self.c3)
        ck, cm = split_pow2(cv, self.grp)
        is_a = t < self.starts[1]
        is_b = t < self.starts[2]
        group = jnp.where(is_a, a, jnp.where(is_b, bg, cg))
        slot = jnp.where(is_a, 0, jnp.where(is_b, (bv + 1) * self.blk, cm * self.blk + ck + 1))
        local = jnp.where(is_a, a, jnp.where(is_b, b, c))
        count = jnp.where(is_a, self.counts[0], jnp.where(is_b, self.counts[1], self.counts[2]))
        return jnp.where(local < count, group * self.period, -(1 << 20)), slot


def flip(s, r):
    step = 1
    while step <= r:
        if r & step:
            s = s + step * (1 - 2 * ((s // step) % 2))
        step *= 2
    return s


def kernel(
    plan, q_hbm, k_hbm, v_hbm, valid_hbm, offs_hbm, w_hbm, o_ref,
    qkv_ref, valid_ref, offs_ref, w_ref,
    buf_a, buf_b, buf_c, snd_a, snd_b, snd_c, snd_q, own_q, got_q, ret_s, ret_r, own_o, back_hot,
    load, zsend, zrecv, crecv, qsem, asend, arecv, bsend, brecv, fsend, frecv, rsem,
):
    G, B, N = plan.grp, plan.blk, plan.n
    R = plan.total
    K = G // 2
    H = plan.half
    gi, bi, si = lax.axis_index("grp"), lax.axis_index("blk"), lax.axis_index("set")
    core = gi % 2
    partner = gi + 1 - 2 * core
    even = si % 2 == 0

    def peer(sx, sy):
        return (lax.rem(gi + 2 * sx, G), lax.rem(bi + sy, B), si)


    across = [(sx, sy) for sx in range(K) for sy in range(B) if sx or sy]

    barrier = pltpu.get_barrier_semaphore()

    def greet(device):
        pl.semaphore_signal(barrier, inc=1, device_id=device, device_id_type=MESH)

    for r in range(N - 1, 0, -1):
        greet((gi, bi, flip(si, r)))
    for sx, sy in across:
        greet(peer(sx, sy))
    greet((partner, bi, si))

    load_offs = pltpu.make_async_copy(offs_hbm, offs_ref, load.at[0])
    load_valid = pltpu.make_async_copy(valid_hbm, valid_ref, load.at[1])
    load_qkv = [pltpu.make_async_copy(src, qkv_ref.at[n], load.at[2]) for n, src in enumerate((q_hbm, k_hbm, v_hbm))]
    load_w = pltpu.make_async_copy(w_hbm, w_ref, load.at[3])
    for copy in (load_offs, load_valid, *load_qkv, load_w):
        copy.start()
    load_offs.wait()
    load_valid.wait()
    pltpu.make_async_copy(qkv_ref, qkv_ref, load.at[2]).wait()

    lane = lax.broadcasted_iota(jnp.int32, (R, LANES), 1)
    left = lane < HD
    base, slot = plan.source(lax.broadcasted_iota(jnp.int32, (R, plan.rows), 0))
    token = lax.broadcasted_iota(jnp.int32, (R, plan.rows), 1)
    valid_row = (valid_ref[...] > 0).astype(jnp.float32)
    flag_lane = lax.broadcasted_iota(jnp.int32, (UNIT, LANES), 1)

    moved = {}
    columns = {}
    for h in range(HEAD_COUNT):
        cols = slice((h // 2) * LANES, (h // 2 + 1) * LANES)
        packed = jnp.concatenate([qkv_ref[n, :, cols] for n in range(3)], axis=1)
        hit = token == base + ((slot + offs_ref[1, h]) & (plan.period - 1))
        onehot = jnp.where(hit, jnp.float32(1), jnp.float32(0))
        moved[h] = jnp.dot(onehot.astype(jnp.bfloat16), packed, preferred_element_type=jnp.float32)
        columns[h] = jnp.sum(onehot * valid_row, axis=1, keepdims=True)

    def piece(h, which):
        return moved[h][:, which * LANES:(which + 1) * LANES]

    def fold(x, keep):
        low = x[H:]
        if R < 2 * H:
            low = jnp.concatenate([low, jnp.zeros((2 * H - R, LANES), low.dtype)], axis=0)
        return jnp.where(keep, x[:H], pltpu.roll(low, HD, 1))

    def unfold(x):
        x = x.astype(jnp.float32)
        return jnp.concatenate([x, pltpu.roll(x, HD, 1)[:R - H]], axis=0).astype(jnp.bfloat16)

    packs = []
    for number, (a, b, c) in enumerate(SETS):
        flags = jnp.zeros((UNIT, LANES), jnp.float32)
        for j, h in enumerate((a, b, c)):
            for u in range(R // UNIT):
                flags = jnp.where(
                    flag_lane == u * FLAG_STRIDE + j, columns[h][u * UNIT:(u + 1) * UNIT, :], flags
                )
        turned = pltpu.roll(piece(c, 2), HD, 1)
        mixed = jnp.where(left, piece(c, 1), turned) if number == 0 else jnp.where(left, turned, piece(c, 1))
        packs.append(
            (
                jnp.where(left, piece(a, 1), piece(b, 1)),
                jnp.where(left, piece(a, 2), piece(b, 2)),
                mixed,
                jnp.where(left, piece(a, 0), piece(b, 0)) * 0.125,
                piece(c, 0) * 0.125,
                flags,
                fold(piece(c, 0) * 0.125, left[:H] if number == 0 else ~left[:H]),
            )
        )
    mine = [jnp.where(even, x, y).astype(jnp.bfloat16) for x, y in zip(*packs)]
    other = [jnp.where(even, y, x).astype(jnp.bfloat16) for x, y in zip(*packs)]
    a_end, b_end = plan.starts[1], plan.starts[2]
    for j in range(PARTS):
        buf_a[0, 0, 0, j] = mine[j][:a_end]
        snd_a[j] = other[j][:a_end]
        buf_b[0, 0, j] = mine[j][a_end:b_end]
        snd_b[j] = other[j][a_end:b_end]
        buf_c[0, j] = mine[j][b_end:]
        snd_c[j] = other[j][b_end:]
    buf_a[0, 0, 0, PARTS, 0:UNIT] = mine[5]
    snd_a[PARTS, 0:UNIT] = other[5]
    for j in range(2):
        own_q[j] = mine[3 + j]
    snd_q[0:R] = other[3]
    snd_q[R:R + H] = other[6]

    pl.semaphore_wait(barrier, (N - 1) + len(across) + 1)

    heads = (slice(0, 2), slice(2, 3))
    line_sem = (lambda r: zrecv.at[0, r - 1], lambda r: zrecv.at[1, r - 1], lambda r: zrecv.at[2, r - 1])

    def line_ref(part, r):
        if part == 0:
            return buf_a.at[0, 0, r]
        if part < 3:
            return buf_b.at[0, r, heads[part - 1]]
        return buf_c.at[r, heads[part - 3]]

    def zcopy(part, r):
        sent = snd_a if part == 0 else (snd_b if part < 3 else snd_c).at[heads[(part - 1) % 2]]
        return pltpu.make_async_remote_copy(
            src_ref=sent if r % 2 else line_ref(part, 0),
            dst_ref=line_ref(part, r),
            send_sem=zsend.at[part],
            recv_sem=line_sem[part](r) if part < 3 else crecv.at[part - 3],
            device_id=(gi, bi, flip(si, r)), device_id_type=MESH,
        )

    def line_sent(part):
        rest = slice(1, N)
        ref = (
            buf_a.at[0, 0, rest] if part == 0
            else buf_b.at[0, rest, heads[part - 1]] if part < 3
            else buf_c.at[rest, heads[part - 3]]
        )
        pltpu.make_async_copy(ref, ref, zsend.at[part]).wait()

    def qcopy():
        return pltpu.make_async_remote_copy(
            src_ref=snd_q, dst_ref=got_q, send_sem=qsem.at[0], recv_sem=qsem.at[1],
            device_id=(gi, bi, flip(si, 1)), device_id_type=MESH,
        )

    def acopy(x, y, r):
        return pltpu.make_async_remote_copy(
            src_ref=buf_a.at[0, 0, r], dst_ref=buf_a.at[2 * x, y, r],
            send_sem=asend.at[x, y], recv_sem=arecv.at[x, y],
            device_id=peer((K - x) % K, (B - y) % B), device_id_type=MESH,
        )

    def bcopy(y, r, j):
        return pltpu.make_async_remote_copy(
            src_ref=buf_b.at[0, r, heads[j]], dst_ref=buf_b.at[y, r, heads[j]],
            send_sem=bsend.at[j, y - 1], recv_sem=brecv.at[j, y - 1],
            device_id=peer(0, B - y), device_id_type=MESH,
        )

    def fcopy(x, y):
        return pltpu.make_async_remote_copy(
            src_ref=buf_a.at[2 * x, y], dst_ref=buf_a.at[2 * x + 1, y],
            send_sem=fsend.at[x], recv_sem=frecv.at[x],
            device_id=(partner, bi, si), device_id_type=MESH,
        )

    def rcopy(j):
        rows = (slice(0, R), slice(R, R + H))[j]
        return pltpu.make_async_remote_copy(
            src_ref=ret_s.at[rows], dst_ref=ret_r.at[rows], send_sem=rsem.at[0, j], recv_sem=rsem.at[1, j],
            device_id=(gi, bi, flip(si, 1)), device_id_type=MESH,
        )

    def arrived(ref, sem):
        pltpu.make_async_copy(ref, ref, sem).wait()

    def spread_a(r):
        for x, y in across:
            acopy(x, y, r).start()

    def spread_b(r, j):
        for y in range(1, B):
            bcopy(y, r, j).start()

    order = list(range(N - 1, 0, -1))

    def send_line(part):
        for r in order:
            zcopy(part, r).start()

    send_line(0)
    spread_a(0)
    send_line(1)
    spread_b(0, 0)
    send_line(2)
    spread_b(0, 1)
    qcopy().start()
    send_line(3)
    send_line(4)

    token = lax.broadcasted_iota(jnp.int32, (plan.rows, R), 0)
    base, slot = plan.source(lax.broadcasted_iota(jnp.int32, (plan.rows, R), 1))
    for h in range(HEAD_COUNT):
        hit = token == base + ((slot + offs_ref[1, h]) & (plan.period - 1))
        back_hot[h] = jnp.where(hit, jnp.float32(1), jnp.float32(0)).astype(jnp.bfloat16)

    for r in range(1, N):
        zcopy(0, r).wait_recv()
        spread_a(r)
    fcopy(0, 0).start()
    for r in range(1, N):
        zcopy(1, r).wait_recv()
        spread_b(r, 0)
    for r in range(1, N):
        zcopy(2, r).wait_recv()
        spread_b(r, 1)
    for x, y in across:
        arrived(buf_a.at[2 * x, y], arecv.at[x, y])
        fcopy(x, y).start()

    head_pick = lax.broadcasted_iota(jnp.int32, (FLAG_STRIDE, LANES), 1) & (FLAG_STRIDE - 1)
    head_pick = head_pick == lax.broadcasted_iota(jnp.int32, (FLAG_STRIDE, LANES), 0)
    head_pick = jnp.where(head_pick, jnp.float32(1), jnp.float32(0)).astype(jnp.bfloat16)

    def gather(level, at):
        pieces = []
        for u in range(plan.units[0]):
            rows = slice(u * UNIT, (u + 1) * UNIT)
            part = (buf_a[0, 0, :, at, rows], buf_a[0, :, :, at, rows], buf_a[:, :, :, at, rows])[level]
            pieces.append(part.reshape(-1, LANES))
        if level < 2:
            for u in range(plan.units[1]):
                rows = slice(u * UNIT, (u + 1) * UNIT)
                part = buf_b[0, :, at, rows] if level == 0 else buf_b[:, :, at, rows]
                pieces.append(part.reshape(-1, LANES))
        if level == 0:
            for u in range(plan.units[2]):
                pieces.append(buf_c[:, at, u * UNIT:(u + 1) * UNIT].reshape(-1, LANES))
        return pieces[0] if len(pieces) == 1 else jnp.concatenate(pieces, axis=0)

    def level_attend(level):
        M = (R, b_end, a_end)[level]
        tiles = M // UNIT
        devices = (N, B * N, G * B * N)[level]
        per_unit = devices * UNIT
        rows = slice(0, UNIT)
        at = PARTS
        tall = (buf_a[0, 0, :, at, rows], buf_a[0, :, :, at, rows], buf_a[:, :, :, at, rows])[level]
        tall = tall.reshape(per_unit, LANES).astype(jnp.float32)
        unit_lane = lax.broadcasted_iota(jnp.int32, (per_unit, LANES), 1) // FLAG_STRIDE
        tall = [jnp.where(unit_lane == u, tall, 0.0).astype(jnp.bfloat16) for u in range(tiles)]
        tall = tall[0] if tiles == 1 else jnp.concatenate(tall, axis=0)
        ok = lax.dot_general(
            head_pick, tall, (((1,), (1,)), ((), ())), preferred_element_type=jnp.float32
        )
        keys = per_unit * tiles
        row = lax.broadcasted_iota(jnp.int32, (2 * M, keys), 0)
        who = jnp.where(row < M, 0, 1)
        t = row - who * M
        spot = (t // UNIT) * per_unit + (t % UNIT) + who * UNIT
        own = lax.broadcasted_iota(jnp.int32, (2 * M, keys), 1) == spot
        half_lane = lax.broadcasted_iota(jnp.int32, (2 * M, LANES), 1) < HD
        value_lane = half_lane != even
        contract = (((1,), (1,)), ((), ()))
        zero = jnp.zeros((2 * M, LANES), jnp.bfloat16)

        def query(j):
            return jnp.concatenate([own_q[j, 0:M], got_q[0:M] if j == 0 else got_single[0:M]], axis=0)

        def run(parts):
            scores = []
            if 0 in parts:
                q = query(0)
                both = jnp.concatenate([jnp.where(half_lane, q, zero), jnp.where(half_lane, zero, q)], axis=0)
                both = lax.dot_general(both, gather(level, 0), contract, preferred_element_type=jnp.float32)
                scores += [both[:2 * M], both[2 * M:]]
            if 1 in parts:
                single = gather(level, 2)
                q = jnp.where(value_lane, zero, query(1))
                scores.append(lax.dot_general(q, single, contract, preferred_element_type=jnp.float32))
            first = 0 if 0 in parts else 2
            scores = [jnp.where(own | (ok[first + n:first + n + 1, :] > 0.5), s, NEG) for n, s in enumerate(scores)]
            tops = [jnp.max(s, axis=1, keepdims=True) for s in scores]
            weights = [jnp.exp(s - top) for s, top in zip(scores, tops)]
            probs = [w.astype(jnp.bfloat16) for w in weights]
            results = []
            if 0 in parts:
                pair = jnp.dot(jnp.concatenate(probs[:2], axis=0), gather(level, 1), preferred_element_type=jnp.float32)
            if 1 in parts:
                alone = jnp.dot(probs[-1], single, preferred_element_type=jnp.float32)
            totals = [jnp.sum(w, axis=1, keepdims=True) for w in weights]
            lses = [top + jnp.log(total) for top, total in zip(tops, totals)]
            if 0 in parts:
                results.append(
                    (
                        jnp.where(half_lane, pair[:2 * M] / totals[0], pair[2 * M:] / totals[1]),
                        jnp.where(half_lane, lses[0], lses[1]),
                    )
                )
            if 1 in parts:
                results.append((alone / totals[-1], jnp.broadcast_to(lses[-1], (2 * M, LANES))))
            return results

        return run

    def combine(levels):
        top = functools.reduce(jnp.maximum, [lse for _, lse in levels])
        shares = [jnp.exp(lse - top) for _, lse in levels]
        return sum(s * o for s, (o, _) in zip(shares, levels)) / sum(shares)

    qcopy().wait_recv()
    for x in range(K):
        arrived(buf_a.at[2 * x + 1], frecv.at[x])
    got_single = unfold(got_q[R:R + H])
    outer, middle, dense = level_attend(2), level_attend(1), level_attend(0)
    third = outer((0, 1))
    value_half = left[:H] != even
    for j in range(2):
        for y in range(1, B):
            arrived(buf_b.at[y, :, heads[j]], brecv.at[j, y - 1])
        second = middle((j,))[0]
        arrived(buf_c.at[1:N, heads[j]], crecv.at[j])
        first = dense((j,))[0]
        for who in (1, 0):
            (o1, l1), (o2, l2), (o3, l3) = [
                tuple(x[who * m:(who + 1) * m] for x in level)
                for level, m in ((first, R), (second, b_end), (third[j], a_end))
            ]
            mixed = jnp.concatenate(
                [
                    combine([(o1[:a_end], l1[:a_end]), (o2[:a_end], l2[:a_end]), (o3, l3)]),
                    combine([(o1[a_end:b_end], l1[a_end:b_end]), (o2[a_end:], l2[a_end:])]),
                    o1[b_end:],
                ],
                axis=0,
            )
            if who == 0:
                own_o[j] = mixed.astype(jnp.bfloat16)
            else:
                if j == 0:
                    ret_s[0:R] = mixed.astype(jnp.bfloat16)
                else:
                    ret_s[R:R + H] = fold(mixed, value_half).astype(jnp.bfloat16)
                rcopy(j).start()
    for part in range(5):
        line_sent(part)
    qcopy().wait_send()
    for x, y in across:
        arrived(buf_a.at[0, 0], asend.at[x, y])
    for j in range(2):
        for y in range(1, B):
            arrived(buf_b.at[0, :, heads[j]], bsend.at[j, y - 1])
    for x in range(K):
        arrived(buf_a.at[2 * x], fsend.at[x])
    load_w.wait()
    for j in range(2):
        rcopy(j).wait_recv()

    got = (ret_r[0:R], unfold(ret_r[R:R + H]))
    sets = [
        (jnp.where(even, own_o[j], got[j]), jnp.where(even, got[j], own_o[j])) for j in range(2)
    ]
    (zero_pair, one_pair), (zero_single, one_single) = sets
    singles = jnp.where(left, one_single, zero_single)
    out_left = lax.broadcasted_iota(jnp.int32, (plan.rows, LANES), 1) < HD
    attention, weights = [], []
    for value, (a, b) in ((zero_pair, SETS[0][:2]), (one_pair, SETS[1][:2]), (singles, (SETS[1][2], SETS[0][2]))):
        back = [jnp.dot(back_hot[h], value, preferred_element_type=jnp.float32) for h in (a, b)]
        attention.append(jnp.where(out_left, back[0], back[1]).astype(jnp.bfloat16))
        weights += [w_ref[a * HD:(a + 1) * HD, :], w_ref[b * HD:(b + 1) * HD, :]]
    attention = jnp.concatenate(attention, axis=1)
    weights = jnp.concatenate(weights, axis=0)
    o_ref[...] = jnp.dot(attention, weights, preferred_element_type=jnp.float32).astype(o_ref.dtype)

    for j in range(2):
        rcopy(j).wait_send()


def solution(mesh):
    G, B, N = mesh.shape["grp"], mesh.shape["blk"], mesh.shape["set"]

    def per_device(queries, keys, values, valid, offsets, w_out):
        rows, width = queries.shape
        plan = Plan(G, B, N, rows)
        vmem = pl.BlockSpec(memory_space=pltpu.VMEM)
        anywhere = pl.BlockSpec(memory_space=pl.ANY)
        dma = pltpu.SemaphoreType.DMA
        ra, rb, rc = plan.sizes
        R = plan.total
        bf16 = jnp.bfloat16
        return pl.pallas_call(
            functools.partial(kernel, plan),
            out_shape=jax.ShapeDtypeStruct((rows, w_out.shape[1]), bf16),
            in_specs=[anywhere] * 6,
            out_specs=vmem,
            scratch_shapes=[
                pltpu.VMEM((3, rows, width), bf16),
                pltpu.VMEM((1, rows), jnp.int32),
                pltpu.SMEM(offsets.shape, jnp.int32),
                pltpu.VMEM(w_out.shape, bf16),
                pltpu.VMEM((G, B, N, PARTS + 1, ra, LANES), bf16),
                pltpu.VMEM((B, N, PARTS, rb, LANES), bf16),
                pltpu.VMEM((N, PARTS, rc, LANES), bf16),
                pltpu.VMEM((PARTS + 1, ra, LANES), bf16),
                pltpu.VMEM((PARTS, rb, LANES), bf16),
                pltpu.VMEM((PARTS, rc, LANES), bf16),
                pltpu.VMEM((R + plan.half, LANES), bf16),
                pltpu.VMEM((2, R, LANES), bf16),
                pltpu.VMEM((R + plan.half, LANES), bf16),
                pltpu.VMEM((R + plan.half, LANES), bf16),
                pltpu.VMEM((R + plan.half, LANES), bf16),
                pltpu.VMEM((2, R, LANES), bf16),
                pltpu.VMEM((HEAD_COUNT, rows, R), bf16),
                dma((4,)),
                dma((5,)),
                dma((3, N - 1)),
                dma((2,)),
                dma((2,)),
                dma((G // 2, B)),
                dma((G // 2, B)),
                dma((2, B - 1)),
                dma((2, B - 1)),
                dma((G // 2,)),
                dma((G // 2,)),
                dma((2, 2)),
            ],
            compiler_params=pltpu.CompilerParams(
                collective_id=0, has_side_effects=True, vmem_limit_bytes=60 * 1024 * 1024
            ),
        )(queries, keys, values, valid.reshape(1, rows), offsets, w_out)

    rows_spec = P(("grp", "blk", "set"), None)
    return jax.shard_map(
        per_device,
        mesh=mesh,
        in_specs=(rows_spec, rows_spec, rows_spec, P(("grp", "blk", "set")), P(), P()),
        out_specs=rows_spec,
        check_vma=False,
    )
```

```python
import functools

import jax
import jax.numpy as jnp
from jax import lax
from jax.experimental import pallas as pl
from jax.experimental.pallas import tpu as pltpu
from jax.sharding import PartitionSpec as P

HEAD_COUNT = 6
HD = 64
LANES = 128
UNIT = 16
FLAG_STRIDE = 8
CHUNKS = HEAD_COUNT * HD // LANES
SETS = ((0, 3, 4), (2, 1, 5))
PARTS = 3
MESH = pl.DeviceIdType.MESH
NEG = -1e30


def units(count):
    return -(-count // UNIT)


def split_pow2(x, size):
    shift = size.bit_length() - 1
    return lax.shift_right_logical(x, shift), x & (size - 1)


class Plan:
    def __init__(self, grp, blk, n, rows):
        self.grp, self.blk, self.n, self.rows = grp, blk, n, rows
        self.period = grp * blk
        self.c3 = rows // self.period
        c2 = rows // blk
        self.counts = (self.c3, c2 - self.c3, rows - c2)
        self.units = tuple(units(c) for c in self.counts)
        self.sizes = tuple(u * UNIT for u in self.units)
        self.starts = (0, self.sizes[0], self.sizes[0] + self.sizes[1])
        self.total = sum(self.sizes)
        self.half = units(-(-self.total // 2)) * UNIT

    def source(self, t):
        a = t
        b = t - self.starts[1]
        c = t - self.starts[2]
        bv, bg = split_pow2(b, self.c3)
        cv, cg = split_pow2(c, self.c3)
        ck, cm = split_pow2(cv, self.grp)
        is_a = t < self.starts[1]
        is_b = t < self.starts[2]
        group = jnp.where(is_a, a, jnp.where(is_b, bg, cg))
        slot = jnp.where(is_a, 0, jnp.where(is_b, (bv + 1) * self.blk, cm * self.blk + ck + 1))
        local = jnp.where(is_a, a, jnp.where(is_b, b, c))
        count = jnp.where(is_a, self.counts[0], jnp.where(is_b, self.counts[1], self.counts[2]))
        return jnp.where(local < count, group * self.period, -(1 << 20)), slot


def flip(s, r):
    step = 1
    while step <= r:
        if r & step:
            s = s + step * (1 - 2 * ((s // step) % 2))
        step *= 2
    return s


def unfold(plan, x):
    x = x.astype(jnp.float32)
    low = pltpu.roll(x, HD, 1)[:plan.total - plan.half]
    return jnp.concatenate([x, low], axis=0).astype(jnp.bfloat16)


def kernel(
    plan, q_hbm, k_hbm, v_hbm, valid_hbm, offs_hbm, own_o, ret_r, back_hot,
    qkv_ref, valid_ref, offs_ref,
    buf_a, buf_b, buf_c, snd_a, snd_b, snd_c, snd_q, own_q, got_q, ret_s,
    load, zsend, zrecv, crecv, qsem, asend, arecv, bsend, brecv, fsend, frecv, rsem,
):
    G, B, N = plan.grp, plan.blk, plan.n
    R = plan.total
    K = G // 2
    H = plan.half
    gi, bi, si = lax.axis_index("grp"), lax.axis_index("blk"), lax.axis_index("set")
    core = gi % 2
    partner = gi + 1 - 2 * core
    even = si % 2 == 0

    def peer(sx, sy):
        return (lax.rem(gi + 2 * sx, G), lax.rem(bi + sy, B), si)


    across = [(sx, sy) for sx in range(K) for sy in range(B) if sx or sy]

    barrier = pltpu.get_barrier_semaphore()

    def greet(device):
        pl.semaphore_signal(barrier, inc=1, device_id=device, device_id_type=MESH)

    for r in range(N - 1, 0, -1):
        greet((gi, bi, flip(si, r)))
    for sx, sy in across:
        greet(peer(sx, sy))
    greet((partner, bi, si))

    load_offs = pltpu.make_async_copy(offs_hbm, offs_ref, load.at[0])
    load_valid = pltpu.make_async_copy(valid_hbm, valid_ref, load.at[1])
    load_qkv = [pltpu.make_async_copy(src, qkv_ref.at[n], load.at[2]) for n, src in enumerate((q_hbm, k_hbm, v_hbm))]
    for copy in (load_offs, load_valid, *load_qkv):
        copy.start()
    load_offs.wait()
    load_valid.wait()
    pltpu.make_async_copy(qkv_ref, qkv_ref, load.at[2]).wait()

    lane = lax.broadcasted_iota(jnp.int32, (R, LANES), 1)
    left = lane < HD
    base, slot = plan.source(lax.broadcasted_iota(jnp.int32, (R, plan.rows), 0))
    token = lax.broadcasted_iota(jnp.int32, (R, plan.rows), 1)
    valid_row = (valid_ref[...] > 0).astype(jnp.float32)
    flag_lane = lax.broadcasted_iota(jnp.int32, (UNIT, LANES), 1)

    moved = {}
    columns = {}
    for h in range(HEAD_COUNT):
        cols = slice((h // 2) * LANES, (h // 2 + 1) * LANES)
        packed = jnp.concatenate([qkv_ref[n, :, cols] for n in range(3)], axis=1)
        hit = token == base + ((slot + offs_ref[1, h]) & (plan.period - 1))
        onehot = jnp.where(hit, jnp.float32(1), jnp.float32(0))
        moved[h] = jnp.dot(onehot.astype(jnp.bfloat16), packed, preferred_element_type=jnp.float32)
        columns[h] = jnp.sum(onehot * valid_row, axis=1, keepdims=True)

    def piece(h, which):
        return moved[h][:, which * LANES:(which + 1) * LANES]

    def fold(x, keep):
        low = x[H:]
        if R < 2 * H:
            low = jnp.concatenate([low, jnp.zeros((2 * H - R, LANES), low.dtype)], axis=0)
        return jnp.where(keep, x[:H], pltpu.roll(low, HD, 1))

    packs = []
    for number, (a, b, c) in enumerate(SETS):
        flags = jnp.zeros((UNIT, LANES), jnp.float32)
        for j, h in enumerate((a, b, c)):
            for u in range(R // UNIT):
                flags = jnp.where(
                    flag_lane == u * FLAG_STRIDE + j, columns[h][u * UNIT:(u + 1) * UNIT, :], flags
                )
        turned = pltpu.roll(piece(c, 2), HD, 1)
        mixed = jnp.where(left, piece(c, 1), turned) if number == 0 else jnp.where(left, turned, piece(c, 1))
        packs.append(
            (
                jnp.where(left, piece(a, 1), piece(b, 1)),
                jnp.where(left, piece(a, 2), piece(b, 2)),
                mixed,
                jnp.where(left, piece(a, 0), piece(b, 0)) * 0.125,
                piece(c, 0) * 0.125,
                flags,
                fold(piece(c, 0) * 0.125, left[:H] if number == 0 else ~left[:H]),
            )
        )
    mine = [jnp.where(even, x, y).astype(jnp.bfloat16) for x, y in zip(*packs)]
    other = [jnp.where(even, y, x).astype(jnp.bfloat16) for x, y in zip(*packs)]
    a_end, b_end = plan.starts[1], plan.starts[2]
    for j in range(PARTS):
        buf_a[0, 0, 0, j] = mine[j][:a_end]
        snd_a[j] = other[j][:a_end]
        buf_b[0, 0, j] = mine[j][a_end:b_end]
        snd_b[j] = other[j][a_end:b_end]
        buf_c[0, j] = mine[j][b_end:]
        snd_c[j] = other[j][b_end:]
    buf_a[0, 0, 0, PARTS, 0:UNIT] = mine[5]
    snd_a[PARTS, 0:UNIT] = other[5]
    for j in range(2):
        own_q[j] = mine[3 + j]
    snd_q[0:R] = other[3]
    snd_q[R:R + H] = other[6]

    pl.semaphore_wait(barrier, (N - 1) + len(across) + 1)

    heads = (slice(0, 2), slice(2, 3))
    line_sem = (lambda r: zrecv.at[0, r - 1], lambda r: zrecv.at[1, r - 1], lambda r: zrecv.at[2, r - 1])

    def line_ref(part, r):
        if part == 0:
            return buf_a.at[0, 0, r]
        if part < 3:
            return buf_b.at[0, r, heads[part - 1]]
        return buf_c.at[r, heads[part - 3]]

    def zcopy(part, r):
        sent = snd_a if part == 0 else (snd_b if part < 3 else snd_c).at[heads[(part - 1) % 2]]
        return pltpu.make_async_remote_copy(
            src_ref=sent if r % 2 else line_ref(part, 0),
            dst_ref=line_ref(part, r),
            send_sem=zsend.at[part],
            recv_sem=line_sem[part](r) if part < 3 else crecv.at[part - 3],
            device_id=(gi, bi, flip(si, r)), device_id_type=MESH,
        )

    def line_sent(part):
        rest = slice(1, N)
        ref = (
            buf_a.at[0, 0, rest] if part == 0
            else buf_b.at[0, rest, heads[part - 1]] if part < 3
            else buf_c.at[rest, heads[part - 3]]
        )
        pltpu.make_async_copy(ref, ref, zsend.at[part]).wait()

    def qcopy():
        return pltpu.make_async_remote_copy(
            src_ref=snd_q, dst_ref=got_q, send_sem=qsem.at[0], recv_sem=qsem.at[1],
            device_id=(gi, bi, flip(si, 1)), device_id_type=MESH,
        )

    def acopy(x, y, r):
        return pltpu.make_async_remote_copy(
            src_ref=buf_a.at[0, 0, r], dst_ref=buf_a.at[2 * x, y, r],
            send_sem=asend.at[x, y], recv_sem=arecv.at[x, y],
            device_id=peer((K - x) % K, (B - y) % B), device_id_type=MESH,
        )

    def bcopy(y, r, j):
        return pltpu.make_async_remote_copy(
            src_ref=buf_b.at[0, r, heads[j]], dst_ref=buf_b.at[y, r, heads[j]],
            send_sem=bsend.at[j, y - 1], recv_sem=brecv.at[j, y - 1],
            device_id=peer(0, B - y), device_id_type=MESH,
        )

    def fcopy(x, y):
        return pltpu.make_async_remote_copy(
            src_ref=buf_a.at[2 * x, y], dst_ref=buf_a.at[2 * x + 1, y],
            send_sem=fsend.at[x], recv_sem=frecv.at[x],
            device_id=(partner, bi, si), device_id_type=MESH,
        )

    def rcopy(j):
        rows = (slice(0, R), slice(R, R + H))[j]
        return pltpu.make_async_remote_copy(
            src_ref=ret_s.at[rows], dst_ref=ret_r.at[rows], send_sem=rsem.at[0, j], recv_sem=rsem.at[1, j],
            device_id=(gi, bi, flip(si, 1)), device_id_type=MESH,
        )

    def arrived(ref, sem):
        pltpu.make_async_copy(ref, ref, sem).wait()

    def spread_a(r):
        for x, y in across:
            acopy(x, y, r).start()

    def spread_b(r, j):
        for y in range(1, B):
            bcopy(y, r, j).start()

    order = list(range(N - 1, 0, -1))

    def send_line(part):
        for r in order:
            zcopy(part, r).start()

    send_line(0)
    spread_a(0)
    send_line(1)
    spread_b(0, 0)
    send_line(2)
    spread_b(0, 1)

    token = lax.broadcasted_iota(jnp.int32, (plan.rows, R), 0)
    base, slot = plan.source(lax.broadcasted_iota(jnp.int32, (plan.rows, R), 1))
    for h in range(HEAD_COUNT):
        hit = token == base + ((slot + offs_ref[1, h]) & (plan.period - 1))
        back_hot[h] = jnp.where(hit, jnp.float32(1), jnp.float32(0)).astype(jnp.bfloat16)

    for r in range(1, N):
        zcopy(0, r).wait_recv()
        spread_a(r)
    fcopy(0, 0).start()
    qcopy().start()
    send_line(3)
    send_line(4)
    for r in range(1, N):
        zcopy(1, r).wait_recv()
        spread_b(r, 0)
    for r in range(1, N):
        zcopy(2, r).wait_recv()
        spread_b(r, 1)
    for x, y in across:
        arrived(buf_a.at[2 * x, y], arecv.at[x, y])
        fcopy(x, y).start()

    head_pick = lax.broadcasted_iota(jnp.int32, (FLAG_STRIDE, LANES), 1) & (FLAG_STRIDE - 1)
    head_pick = head_pick == lax.broadcasted_iota(jnp.int32, (FLAG_STRIDE, LANES), 0)
    head_pick = jnp.where(head_pick, jnp.float32(1), jnp.float32(0)).astype(jnp.bfloat16)

    def gather(level, at):
        pieces = []
        for u in range(plan.units[0]):
            rows = slice(u * UNIT, (u + 1) * UNIT)
            part = (buf_a[0, 0, :, at, rows], buf_a[0, :, :, at, rows], buf_a[:, :, :, at, rows])[level]
            pieces.append(part.reshape(-1, LANES))
        if level < 2:
            for u in range(plan.units[1]):
                rows = slice(u * UNIT, (u + 1) * UNIT)
                part = buf_b[0, :, at, rows] if level == 0 else buf_b[:, :, at, rows]
                pieces.append(part.reshape(-1, LANES))
        if level == 0:
            for u in range(plan.units[2]):
                pieces.append(buf_c[:, at, u * UNIT:(u + 1) * UNIT].reshape(-1, LANES))
        return pieces[0] if len(pieces) == 1 else jnp.concatenate(pieces, axis=0)

    def level_attend(level):
        M = (R, b_end, a_end)[level]
        tiles = M // UNIT
        devices = (N, B * N, G * B * N)[level]
        per_unit = devices * UNIT
        rows = slice(0, UNIT)
        at = PARTS
        tall = (buf_a[0, 0, :, at, rows], buf_a[0, :, :, at, rows], buf_a[:, :, :, at, rows])[level]
        tall = tall.reshape(per_unit, LANES).astype(jnp.float32)
        unit_lane = lax.broadcasted_iota(jnp.int32, (per_unit, LANES), 1) // FLAG_STRIDE
        tall = [jnp.where(unit_lane == u, tall, 0.0).astype(jnp.bfloat16) for u in range(tiles)]
        tall = tall[0] if tiles == 1 else jnp.concatenate(tall, axis=0)
        ok = lax.dot_general(
            head_pick, tall, (((1,), (1,)), ((), ())), preferred_element_type=jnp.float32
        )
        keys = per_unit * tiles
        row = lax.broadcasted_iota(jnp.int32, (2 * M, keys), 0)
        who = jnp.where(row < M, 0, 1)
        t = row - who * M
        spot = (t // UNIT) * per_unit + (t % UNIT) + who * UNIT
        own = lax.broadcasted_iota(jnp.int32, (2 * M, keys), 1) == spot
        half_lane = lax.broadcasted_iota(jnp.int32, (2 * M, LANES), 1) < HD
        value_lane = half_lane != even
        contract = (((1,), (1,)), ((), ()))
        zero = jnp.zeros((2 * M, LANES), jnp.bfloat16)

        def query(j):
            return jnp.concatenate([own_q[j, 0:M], got_q[0:M] if j == 0 else got_single[0:M]], axis=0)

        def run(parts):
            scores = []
            if 0 in parts:
                q = query(0)
                both = jnp.concatenate([jnp.where(half_lane, q, zero), jnp.where(half_lane, zero, q)], axis=0)
                both = lax.dot_general(both, gather(level, 0), contract, preferred_element_type=jnp.float32)
                scores += [both[:2 * M], both[2 * M:]]
            if 1 in parts:
                single = gather(level, 2)
                q = jnp.where(value_lane, zero, query(1))
                scores.append(lax.dot_general(q, single, contract, preferred_element_type=jnp.float32))
            first = 0 if 0 in parts else 2
            scores = [jnp.where(own | (ok[first + n:first + n + 1, :] > 0.5), s, NEG) for n, s in enumerate(scores)]
            tops = [jnp.max(s, axis=1, keepdims=True) for s in scores]
            weights = [jnp.exp(s - top) for s, top in zip(scores, tops)]
            probs = [w.astype(jnp.bfloat16) for w in weights]
            results = []
            if 0 in parts:
                pair = jnp.dot(jnp.concatenate(probs[:2], axis=0), gather(level, 1), preferred_element_type=jnp.float32)
            if 1 in parts:
                alone = jnp.dot(probs[-1], single, preferred_element_type=jnp.float32)
            totals = [jnp.sum(w, axis=1, keepdims=True) for w in weights]
            lses = [top + jnp.log(total) for top, total in zip(tops, totals)]
            if 0 in parts:
                results.append(
                    (
                        jnp.where(half_lane, pair[:2 * M] / totals[0], pair[2 * M:] / totals[1]),
                        jnp.where(half_lane, lses[0], lses[1]),
                    )
                )
            if 1 in parts:
                results.append((alone / totals[-1], jnp.broadcast_to(lses[-1], (2 * M, LANES))))
            return results

        return run

    def combine(levels):
        top = functools.reduce(jnp.maximum, [lse for _, lse in levels])
        shares = [jnp.exp(lse - top) for _, lse in levels]
        return sum(s * o for s, (o, _) in zip(shares, levels)) / sum(shares)

    qcopy().wait_recv()
    for x in range(K):
        arrived(buf_a.at[2 * x + 1], frecv.at[x])
    got_single = unfold(plan, got_q[R:R + H])
    outer, middle, dense = level_attend(2), level_attend(1), level_attend(0)
    third = outer((0, 1))
    value_half = left[:H] != even
    for j in range(2):
        for y in range(1, B):
            arrived(buf_b.at[y, :, heads[j]], brecv.at[j, y - 1])
        second = middle((j,))[0]
        arrived(buf_c.at[1:N, heads[j]], crecv.at[j])
        first = dense((j,))[0]
        for who in (1, 0):
            (o1, l1), (o2, l2), (o3, l3) = [
                tuple(x[who * m:(who + 1) * m] for x in level)
                for level, m in ((first, R), (second, b_end), (third[j], a_end))
            ]
            mixed = jnp.concatenate(
                [
                    combine([(o1[:a_end], l1[:a_end]), (o2[:a_end], l2[:a_end]), (o3, l3)]),
                    combine([(o1[a_end:b_end], l1[a_end:b_end]), (o2[a_end:], l2[a_end:])]),
                    o1[b_end:],
                ],
                axis=0,
            )
            if who == 0:
                own_o[j] = mixed.astype(jnp.bfloat16)
            else:
                if j == 0:
                    ret_s[0:R] = mixed.astype(jnp.bfloat16)
                else:
                    ret_s[R:R + H] = fold(mixed, value_half).astype(jnp.bfloat16)
                rcopy(j).start()
    for part in range(5):
        line_sent(part)
    qcopy().wait_send()
    for x, y in across:
        arrived(buf_a.at[0, 0], asend.at[x, y])
    for j in range(2):
        for y in range(1, B):
            arrived(buf_b.at[0, :, heads[j]], bsend.at[j, y - 1])
    for x in range(K):
        arrived(buf_a.at[2 * x], fsend.at[x])
    for j in range(2):
        rcopy(j).wait_recv()

    for j in range(2):
        rcopy(j).wait_send()


def project(plan, own_o, ret_r, back_hot, w_ref, o_ref):
    R, H = plan.total, plan.half
    even = lax.axis_index("set") % 2 == 0
    left = lax.broadcasted_iota(jnp.int32, (R, LANES), 1) < HD
    got = (ret_r[0:R], unfold(plan, ret_r[R:R + H]))
    sets = [
        (jnp.where(even, own_o[j], got[j]), jnp.where(even, got[j], own_o[j])) for j in range(2)
    ]
    (zero_pair, one_pair), (zero_single, one_single) = sets
    singles = jnp.where(left, one_single, zero_single)
    out_left = lax.broadcasted_iota(jnp.int32, (plan.rows, LANES), 1) < HD
    attention, weights = [], []
    for value, (a, b) in ((zero_pair, SETS[0][:2]), (one_pair, SETS[1][:2]), (singles, (SETS[1][2], SETS[0][2]))):
        back = [jnp.dot(back_hot[h], value, preferred_element_type=jnp.float32) for h in (a, b)]
        attention.append(jnp.where(out_left, back[0], back[1]).astype(jnp.bfloat16))
        weights += [w_ref[a * HD:(a + 1) * HD, :], w_ref[b * HD:(b + 1) * HD, :]]
    attention = jnp.concatenate(attention, axis=1)
    weights = jnp.concatenate(weights, axis=0)
    o_ref[...] = jnp.dot(attention, weights, preferred_element_type=jnp.float32).astype(o_ref.dtype)


def solution(mesh):
    G, B, N = mesh.shape["grp"], mesh.shape["blk"], mesh.shape["set"]

    def per_device(queries, keys, values, valid, offsets, w_out):
        rows, width = queries.shape
        plan = Plan(G, B, N, rows)
        vmem = pl.BlockSpec(memory_space=pltpu.VMEM)
        anywhere = pl.BlockSpec(memory_space=pl.ANY)
        dma = pltpu.SemaphoreType.DMA
        ra, rb, rc = plan.sizes
        R = plan.total
        bf16 = jnp.bfloat16
        outputs = ((2, R, LANES), (R + plan.half, LANES), (HEAD_COUNT, rows, R))
        attended = pl.pallas_call(
            functools.partial(kernel, plan),
            out_shape=[pltpu.VMEM(shape, bf16) for shape in outputs],
            in_specs=[anywhere] * 5,
            out_specs=[vmem] * 3,
            cost_estimate=pl.CostEstimate(
                flops=4 * rows * rows * N * width * 4, bytes_accessed=4 * rows * width * 2, transcendentals=0
            ),
            scratch_shapes=[
                pltpu.VMEM((3, rows, width), bf16),
                pltpu.VMEM((1, rows), jnp.int32),
                pltpu.SMEM(offsets.shape, jnp.int32),
                pltpu.VMEM((G, B, N, PARTS + 1, ra, LANES), bf16),
                pltpu.VMEM((B, N, PARTS, rb, LANES), bf16),
                pltpu.VMEM((N, PARTS, rc, LANES), bf16),
                pltpu.VMEM((PARTS + 1, ra, LANES), bf16),
                pltpu.VMEM((PARTS, rb, LANES), bf16),
                pltpu.VMEM((PARTS, rc, LANES), bf16),
                pltpu.VMEM((R + plan.half, LANES), bf16),
                pltpu.VMEM((2, R, LANES), bf16),
                pltpu.VMEM((R + plan.half, LANES), bf16),
                pltpu.VMEM((R + plan.half, LANES), bf16),
                dma((3,)),
                dma((5,)),
                dma((3, N - 1)),
                dma((2,)),
                dma((2,)),
                dma((G // 2, B)),
                dma((G // 2, B)),
                dma((2, B - 1)),
                dma((2, B - 1)),
                dma((G // 2,)),
                dma((G // 2,)),
                dma((2, 2)),
            ],
            compiler_params=pltpu.CompilerParams(
                collective_id=0, has_side_effects=True, vmem_limit_bytes=60 * 1024 * 1024
            ),
        )(queries, keys, values, valid.reshape(1, rows), offsets)
        return pl.pallas_call(
            functools.partial(project, plan),
            out_shape=jax.ShapeDtypeStruct((rows, w_out.shape[1]), bf16),
            in_specs=[vmem] * 4,
            out_specs=vmem,
            compiler_params=pltpu.CompilerParams(vmem_limit_bytes=8 * 1024 * 1024),
        )(*attended, w_out)

    rows_spec = P(("grp", "blk", "set"), None)
    return jax.shard_map(
        per_device,
        mesh=mesh,
        in_specs=(rows_spec, rows_spec, rows_spec, P(("grp", "blk", "set")), P(), P()),
        out_specs=rows_spec,
        check_vma=False,
    )
```

```python
import functools

import jax
import jax.numpy as jnp
from jax import lax
from jax.experimental import pallas as pl
from jax.experimental.pallas import tpu as pltpu
from jax.sharding import PartitionSpec as P

HEAD_COUNT = 6
HD = 64
LANES = 128
UNIT = 16
FLAG_STRIDE = 8
CHUNKS = HEAD_COUNT * HD // LANES
SETS = ((0, 3, 4), (2, 1, 5))
PARTS = 3
MESH = pl.DeviceIdType.MESH
NEG = -1e30


def units(count):
    return -(-count // UNIT)


def split_pow2(x, size):
    shift = size.bit_length() - 1
    return lax.shift_right_logical(x, shift), x & (size - 1)


class Plan:
    def __init__(self, grp, blk, n, rows):
        self.grp, self.blk, self.n, self.rows = grp, blk, n, rows
        self.period = grp * blk
        self.c3 = rows // self.period
        c2 = rows // blk
        self.counts = (self.c3, c2 - self.c3, rows - c2)
        self.units = tuple(units(c) for c in self.counts)
        self.sizes = tuple(u * UNIT for u in self.units)
        self.starts = (0, self.sizes[0], self.sizes[0] + self.sizes[1])
        self.total = sum(self.sizes)
        self.half = units(-(-self.total // 2)) * UNIT

    def source(self, t):
        a = t
        b = t - self.starts[1]
        c = t - self.starts[2]
        bv, bg = split_pow2(b, self.c3)
        cv, cg = split_pow2(c, self.c3)
        ck, cm = split_pow2(cv, self.grp)
        is_a = t < self.starts[1]
        is_b = t < self.starts[2]
        group = jnp.where(is_a, a, jnp.where(is_b, bg, cg))
        slot = jnp.where(is_a, 0, jnp.where(is_b, (bv + 1) * self.blk, cm * self.blk + ck + 1))
        local = jnp.where(is_a, a, jnp.where(is_b, b, c))
        count = jnp.where(is_a, self.counts[0], jnp.where(is_b, self.counts[1], self.counts[2]))
        return jnp.where(local < count, group * self.period, -(1 << 20)), slot


def flip(s, r):
    step = 1
    while step <= r:
        if r & step:
            s = s + step * (1 - 2 * ((s // step) % 2))
        step *= 2
    return s


def unfold(plan, x):
    x = x.astype(jnp.float32)
    low = pltpu.roll(x, HD, 1)[:plan.total - plan.half]
    return jnp.concatenate([x, low], axis=0).astype(jnp.bfloat16)


def kernel(
    plan, q_hbm, k_hbm, v_hbm, valid_hbm, offs_hbm, own_o, ret_r, back_hot,
    qkv_ref, valid_ref, offs_ref,
    buf_a, buf_b, buf_c, snd_a, snd_b, snd_c, snd_q, own_q, got_q, ret_s,
    load, zsend, zrecv, crecv, qsem, asend, afirst, arecv, bsend, brecv, fsend, frecv, rsem,
):
    G, B, N = plan.grp, plan.blk, plan.n
    R = plan.total
    K = G // 2
    H = plan.half
    gi, bi, si = lax.axis_index("grp"), lax.axis_index("blk"), lax.axis_index("set")
    core = gi % 2
    partner = gi + 1 - 2 * core
    even = si % 2 == 0

    def peer(sx, sy):
        return (lax.rem(gi + 2 * sx, G), lax.rem(bi + sy, B), si)


    across = [(x, y) for x in range(K) for y in range(B) if x or y]
    near = [(x, y) for x, y in across if not (x and y)]
    diagonal = [(x, y) for x, y in across if x and y]

    barrier = pltpu.get_barrier_semaphore()

    def greet(device):
        pl.semaphore_signal(barrier, inc=1, device_id=device, device_id_type=MESH)

    for r in range(N - 1, 0, -1):
        greet((gi, bi, flip(si, r)))
    for x, y in near:
        greet(peer(x, y))
    greet((partner, bi, si))

    load_offs = pltpu.make_async_copy(offs_hbm, offs_ref, load.at[0])
    load_valid = pltpu.make_async_copy(valid_hbm, valid_ref, load.at[1])
    load_qkv = [pltpu.make_async_copy(src, qkv_ref.at[n], load.at[2]) for n, src in enumerate((q_hbm, k_hbm, v_hbm))]
    for copy in (load_offs, load_valid, *load_qkv):
        copy.start()
    load_offs.wait()
    load_valid.wait()
    pltpu.make_async_copy(qkv_ref, qkv_ref, load.at[2]).wait()

    lane = lax.broadcasted_iota(jnp.int32, (R, LANES), 1)
    left = lane < HD
    base, slot = plan.source(lax.broadcasted_iota(jnp.int32, (R, plan.rows), 0))
    token = lax.broadcasted_iota(jnp.int32, (R, plan.rows), 1)
    valid_row = (valid_ref[...] > 0).astype(jnp.float32)
    flag_lane = lax.broadcasted_iota(jnp.int32, (UNIT, LANES), 1)

    moved = {}
    columns = {}
    for h in range(HEAD_COUNT):
        cols = slice((h // 2) * LANES, (h // 2 + 1) * LANES)
        packed = jnp.concatenate([qkv_ref[n, :, cols] for n in range(3)], axis=1)
        hit = token == base + ((slot + offs_ref[1, h]) & (plan.period - 1))
        onehot = jnp.where(hit, jnp.float32(1), jnp.float32(0))
        moved[h] = jnp.dot(onehot.astype(jnp.bfloat16), packed, preferred_element_type=jnp.float32)
        columns[h] = jnp.sum(onehot * valid_row, axis=1, keepdims=True)

    def piece(h, which):
        return moved[h][:, which * LANES:(which + 1) * LANES]

    def fold(x, keep):
        low = x[H:]
        if R < 2 * H:
            low = jnp.concatenate([low, jnp.zeros((2 * H - R, LANES), low.dtype)], axis=0)
        return jnp.where(keep, x[:H], pltpu.roll(low, HD, 1))

    packs = []
    for number, (a, b, c) in enumerate(SETS):
        flags = jnp.zeros((UNIT, LANES), jnp.float32)
        for j, h in enumerate((a, b, c)):
            for u in range(R // UNIT):
                flags = jnp.where(
                    flag_lane == u * FLAG_STRIDE + j, columns[h][u * UNIT:(u + 1) * UNIT, :], flags
                )
        turned = pltpu.roll(piece(c, 2), HD, 1)
        mixed = jnp.where(left, piece(c, 1), turned) if number == 0 else jnp.where(left, turned, piece(c, 1))
        packs.append(
            (
                jnp.where(left, piece(a, 1), piece(b, 1)),
                jnp.where(left, piece(a, 2), piece(b, 2)),
                mixed,
                jnp.where(left, piece(a, 0), piece(b, 0)) * 0.125,
                piece(c, 0) * 0.125,
                flags,
                fold(piece(c, 0) * 0.125, left[:H] if number == 0 else ~left[:H]),
            )
        )
    mine = [jnp.where(even, x, y).astype(jnp.bfloat16) for x, y in zip(*packs)]
    other = [jnp.where(even, y, x).astype(jnp.bfloat16) for x, y in zip(*packs)]
    a_end, b_end = plan.starts[1], plan.starts[2]
    for j in range(PARTS):
        buf_a[0, 0, 0, j] = mine[j][:a_end]
        snd_a[j] = other[j][:a_end]
        buf_b[0, 0, j] = mine[j][a_end:b_end]
        snd_b[j] = other[j][a_end:b_end]
        buf_c[0, j] = mine[j][b_end:]
        snd_c[j] = other[j][b_end:]
    buf_a[0, 0, 0, PARTS, 0:UNIT] = mine[5]
    snd_a[PARTS, 0:UNIT] = other[5]
    for j in range(2):
        own_q[j] = mine[3 + j]
    snd_q[0:R] = other[3]
    snd_q[R:R + H] = other[6]

    pl.semaphore_wait(barrier, (N - 1) + len(near) + 1)

    heads = (slice(0, 2), slice(2, 3))
    line_sem = (lambda r: zrecv.at[0, r - 1], lambda r: zrecv.at[1, r - 1], lambda r: zrecv.at[2, r - 1])

    def line_ref(part, r):
        if part == 0:
            return buf_a.at[0, 0, r]
        if part < 3:
            return buf_b.at[0, r, heads[part - 1]]
        return buf_c.at[r, heads[part - 3]]

    def zcopy(part, r):
        sent = snd_a if part == 0 else (snd_b if part < 3 else snd_c).at[heads[(part - 1) % 2]]
        return pltpu.make_async_remote_copy(
            src_ref=sent if r % 2 else line_ref(part, 0),
            dst_ref=line_ref(part, r),
            send_sem=zsend.at[part],
            recv_sem=line_sem[part](r) if part < 3 else crecv.at[part - 3],
            device_id=(gi, bi, flip(si, r)), device_id_type=MESH,
        )

    def line_sent(part):
        rest = slice(1, N)
        ref = (
            buf_a.at[0, 0, rest] if part == 0
            else buf_b.at[0, rest, heads[part - 1]] if part < 3
            else buf_c.at[rest, heads[part - 3]]
        )
        pltpu.make_async_copy(ref, ref, zsend.at[part]).wait()

    def qcopy():
        return pltpu.make_async_remote_copy(
            src_ref=snd_q, dst_ref=got_q, send_sem=qsem.at[0], recv_sem=qsem.at[1],
            device_id=(gi, bi, flip(si, 1)), device_id_type=MESH,
        )

    def acopy(x, y, r):
        return pltpu.make_async_remote_copy(
            src_ref=buf_a.at[0, 0, r], dst_ref=buf_a.at[2 * x, y, r],
            send_sem=asend.at[x, y],
            recv_sem=afirst.at[y - 1] if x == 0 and r == 0 else arecv.at[x, y],
            device_id=peer((K - x) % K, (B - y) % B), device_id_type=MESH,
        )

    def bcopy(y, r, j):
        return pltpu.make_async_remote_copy(
            src_ref=buf_b.at[0, r, heads[j]], dst_ref=buf_b.at[y, r, heads[j]],
            send_sem=bsend.at[j, y - 1], recv_sem=brecv.at[j, y - 1],
            device_id=peer(0, B - y), device_id_type=MESH,
        )

    def fcopy(x, y):
        return pltpu.make_async_remote_copy(
            src_ref=buf_a.at[2 * x, y], dst_ref=buf_a.at[2 * x + 1, y],
            send_sem=fsend.at[x], recv_sem=frecv.at[x],
            device_id=(partner, bi, si), device_id_type=MESH,
        )

    def rcopy(j):
        rows = (slice(0, R), slice(R, R + H))[j]
        return pltpu.make_async_remote_copy(
            src_ref=ret_s.at[rows], dst_ref=ret_r.at[rows], send_sem=rsem.at[0, j], recv_sem=rsem.at[1, j],
            device_id=(gi, bi, flip(si, 1)), device_id_type=MESH,
        )

    def arrived(ref, sem):
        pltpu.make_async_copy(ref, ref, sem).wait()

    def spread_a(r, where):
        for x, y in where:
            acopy(x, y, r).start()

    def spread_b(r, j):
        for y in range(1, B):
            bcopy(y, r, j).start()

    order = list(range(N - 1, 0, -1))

    def send_line(part):
        for r in order:
            zcopy(part, r).start()

    send_line(0)
    spread_a(0, near)
    send_line(1)
    spread_b(0, 0)
    send_line(2)
    spread_b(0, 1)

    token = lax.broadcasted_iota(jnp.int32, (plan.rows, R), 0)
    base, slot = plan.source(lax.broadcasted_iota(jnp.int32, (plan.rows, R), 1))
    for h in range(HEAD_COUNT):
        hit = token == base + ((slot + offs_ref[1, h]) & (plan.period - 1))
        back_hot[h] = jnp.where(hit, jnp.float32(1), jnp.float32(0)).astype(jnp.bfloat16)

    for y in range(1, B):
        acopy(0, y, 0).wait_recv()
    spread_a(0, diagonal)
    for r in range(1, N):
        zcopy(0, r).wait_recv()
        spread_a(r, across)
    fcopy(0, 0).start()
    qcopy().start()
    send_line(3)
    send_line(4)
    for r in range(1, N):
        zcopy(1, r).wait_recv()
        spread_b(r, 0)
    for r in range(1, N):
        zcopy(2, r).wait_recv()
        spread_b(r, 1)
    for x, y in across:
        arrived(buf_a.at[2 * x, y] if x else buf_a.at[0, y, 1:N], arecv.at[x, y])
        fcopy(x, y).start()

    head_pick = lax.broadcasted_iota(jnp.int32, (FLAG_STRIDE, LANES), 1) & (FLAG_STRIDE - 1)
    head_pick = head_pick == lax.broadcasted_iota(jnp.int32, (FLAG_STRIDE, LANES), 0)
    head_pick = jnp.where(head_pick, jnp.float32(1), jnp.float32(0)).astype(jnp.bfloat16)

    def gather(level, at):
        pieces = []
        for u in range(plan.units[0]):
            rows = slice(u * UNIT, (u + 1) * UNIT)
            part = (buf_a[0, 0, :, at, rows], buf_a[0, :, :, at, rows], buf_a[:, :, :, at, rows])[level]
            pieces.append(part.reshape(-1, LANES))
        if level < 2:
            for u in range(plan.units[1]):
                rows = slice(u * UNIT, (u + 1) * UNIT)
                part = buf_b[0, :, at, rows] if level == 0 else buf_b[:, :, at, rows]
                pieces.append(part.reshape(-1, LANES))
        if level == 0:
            for u in range(plan.units[2]):
                pieces.append(buf_c[:, at, u * UNIT:(u + 1) * UNIT].reshape(-1, LANES))
        return pieces[0] if len(pieces) == 1 else jnp.concatenate(pieces, axis=0)

    def level_attend(level):
        M = (R, b_end, a_end)[level]
        tiles = M // UNIT
        devices = (N, B * N, G * B * N)[level]
        per_unit = devices * UNIT
        rows = slice(0, UNIT)
        at = PARTS
        tall = (buf_a[0, 0, :, at, rows], buf_a[0, :, :, at, rows], buf_a[:, :, :, at, rows])[level]
        tall = tall.reshape(per_unit, LANES).astype(jnp.float32)
        unit_lane = lax.broadcasted_iota(jnp.int32, (per_unit, LANES), 1) // FLAG_STRIDE
        tall = [jnp.where(unit_lane == u, tall, 0.0).astype(jnp.bfloat16) for u in range(tiles)]
        tall = tall[0] if tiles == 1 else jnp.concatenate(tall, axis=0)
        ok = lax.dot_general(
            head_pick, tall, (((1,), (1,)), ((), ())), preferred_element_type=jnp.float32
        )
        keys = per_unit * tiles
        row = lax.broadcasted_iota(jnp.int32, (2 * M, keys), 0)
        who = jnp.where(row < M, 0, 1)
        t = row - who * M
        spot = (t // UNIT) * per_unit + (t % UNIT) + who * UNIT
        own = lax.broadcasted_iota(jnp.int32, (2 * M, keys), 1) == spot
        half_lane = lax.broadcasted_iota(jnp.int32, (2 * M, LANES), 1) < HD
        value_lane = half_lane != even
        contract = (((1,), (1,)), ((), ()))
        zero = jnp.zeros((2 * M, LANES), jnp.bfloat16)

        def query(j):
            return jnp.concatenate([own_q[j, 0:M], got_q[0:M] if j == 0 else got_single[0:M]], axis=0)

        def run(parts):
            scores = []
            if 0 in parts:
                q = query(0)
                both = jnp.concatenate([jnp.where(half_lane, q, zero), jnp.where(half_lane, zero, q)], axis=0)
                both = lax.dot_general(both, gather(level, 0), contract, preferred_element_type=jnp.float32)
                scores += [both[:2 * M], both[2 * M:]]
            if 1 in parts:
                single = gather(level, 2)
                q = jnp.where(value_lane, zero, query(1))
                scores.append(lax.dot_general(q, single, contract, preferred_element_type=jnp.float32))
            first = 0 if 0 in parts else 2
            scores = [jnp.where(own | (ok[first + n:first + n + 1, :] > 0.5), s, NEG) for n, s in enumerate(scores)]
            tops = [jnp.max(s, axis=1, keepdims=True) for s in scores]
            weights = [jnp.exp(s - top) for s, top in zip(scores, tops)]
            probs = [w.astype(jnp.bfloat16) for w in weights]
            results = []
            if 0 in parts:
                pair = jnp.dot(jnp.concatenate(probs[:2], axis=0), gather(level, 1), preferred_element_type=jnp.float32)
            if 1 in parts:
                alone = jnp.dot(probs[-1], single, preferred_element_type=jnp.float32)
            totals = [jnp.sum(w, axis=1, keepdims=True) for w in weights]
            lses = [top + jnp.log(total) for top, total in zip(tops, totals)]
            if 0 in parts:
                results.append(
                    (
                        jnp.where(half_lane, pair[:2 * M] / totals[0], pair[2 * M:] / totals[1]),
                        jnp.where(half_lane, lses[0], lses[1]),
                    )
                )
            if 1 in parts:
                results.append((alone / totals[-1], jnp.broadcast_to(lses[-1], (2 * M, LANES))))
            return results

        return run

    def combine(levels):
        top = functools.reduce(jnp.maximum, [lse for _, lse in levels])
        shares = [jnp.exp(lse - top) for _, lse in levels]
        return sum(s * o for s, (o, _) in zip(shares, levels)) / sum(shares)

    qcopy().wait_recv()
    for x in range(K):
        arrived(buf_a.at[2 * x + 1], frecv.at[x])
    got_single = unfold(plan, got_q[R:R + H])
    outer, middle, dense = level_attend(2), level_attend(1), level_attend(0)
    third = outer((0, 1))
    value_half = left[:H] != even
    for j in range(2):
        for y in range(1, B):
            arrived(buf_b.at[y, :, heads[j]], brecv.at[j, y - 1])
        second = middle((j,))[0]
        arrived(buf_c.at[1:N, heads[j]], crecv.at[j])
        first = dense((j,))[0]
        for who in (1, 0):
            (o1, l1), (o2, l2), (o3, l3) = [
                tuple(x[who * m:(who + 1) * m] for x in level)
                for level, m in ((first, R), (second, b_end), (third[j], a_end))
            ]
            mixed = jnp.concatenate(
                [
                    combine([(o1[:a_end], l1[:a_end]), (o2[:a_end], l2[:a_end]), (o3, l3)]),
                    combine([(o1[a_end:b_end], l1[a_end:b_end]), (o2[a_end:], l2[a_end:])]),
                    o1[b_end:],
                ],
                axis=0,
            )
            if who == 0:
                own_o[j] = mixed.astype(jnp.bfloat16)
            else:
                if j == 0:
                    ret_s[0:R] = mixed.astype(jnp.bfloat16)
                else:
                    ret_s[R:R + H] = fold(mixed, value_half).astype(jnp.bfloat16)
                rcopy(j).start()
    for part in range(5):
        line_sent(part)
    qcopy().wait_send()
    for x, y in across:
        arrived(buf_a.at[0, 0], asend.at[x, y])
    for j in range(2):
        for y in range(1, B):
            arrived(buf_b.at[0, :, heads[j]], bsend.at[j, y - 1])
    for x in range(K):
        arrived(buf_a.at[2 * x], fsend.at[x])
    for j in range(2):
        rcopy(j).wait_recv()

    for j in range(2):
        rcopy(j).wait_send()


def project(plan, own_o, ret_r, back_hot, w_ref, o_ref):
    R, H = plan.total, plan.half
    even = lax.axis_index("set") % 2 == 0
    left = lax.broadcasted_iota(jnp.int32, (R, LANES), 1) < HD
    got = (ret_r[0:R], unfold(plan, ret_r[R:R + H]))
    sets = [
        (jnp.where(even, own_o[j], got[j]), jnp.where(even, got[j], own_o[j])) for j in range(2)
    ]
    (zero_pair, one_pair), (zero_single, one_single) = sets
    singles = jnp.where(left, one_single, zero_single)
    out_left = lax.broadcasted_iota(jnp.int32, (plan.rows, LANES), 1) < HD
    attention, weights = [], []
    for value, (a, b) in ((zero_pair, SETS[0][:2]), (one_pair, SETS[1][:2]), (singles, (SETS[1][2], SETS[0][2]))):
        back = [jnp.dot(back_hot[h], value, preferred_element_type=jnp.float32) for h in (a, b)]
        attention.append(jnp.where(out_left, back[0], back[1]).astype(jnp.bfloat16))
        weights += [w_ref[a * HD:(a + 1) * HD, :], w_ref[b * HD:(b + 1) * HD, :]]
    attention = jnp.concatenate(attention, axis=1)
    weights = jnp.concatenate(weights, axis=0)
    o_ref[...] = jnp.dot(attention, weights, preferred_element_type=jnp.float32).astype(o_ref.dtype)


def solution(mesh):
    G, B, N = mesh.shape["grp"], mesh.shape["blk"], mesh.shape["set"]

    def per_device(queries, keys, values, valid, offsets, w_out):
        rows, width = queries.shape
        plan = Plan(G, B, N, rows)
        vmem = pl.BlockSpec(memory_space=pltpu.VMEM)
        anywhere = pl.BlockSpec(memory_space=pl.ANY)
        dma = pltpu.SemaphoreType.DMA
        ra, rb, rc = plan.sizes
        R = plan.total
        bf16 = jnp.bfloat16
        outputs = ((2, R, LANES), (R + plan.half, LANES), (HEAD_COUNT, rows, R))
        attended = pl.pallas_call(
            functools.partial(kernel, plan),
            out_shape=[pltpu.VMEM(shape, bf16) for shape in outputs],
            in_specs=[anywhere] * 5,
            out_specs=[vmem] * 3,
            cost_estimate=pl.CostEstimate(
                flops=4 * rows * rows * N * width * 4, bytes_accessed=4 * rows * width * 2, transcendentals=0
            ),
            scratch_shapes=[
                pltpu.VMEM((3, rows, width), bf16),
                pltpu.VMEM((1, rows), jnp.int32),
                pltpu.SMEM(offsets.shape, jnp.int32),
                pltpu.VMEM((G, B, N, PARTS + 1, ra, LANES), bf16),
                pltpu.VMEM((B, N, PARTS, rb, LANES), bf16),
                pltpu.VMEM((N, PARTS, rc, LANES), bf16),
                pltpu.VMEM((PARTS + 1, ra, LANES), bf16),
                pltpu.VMEM((PARTS, rb, LANES), bf16),
                pltpu.VMEM((PARTS, rc, LANES), bf16),
                pltpu.VMEM((R + plan.half, LANES), bf16),
                pltpu.VMEM((2, R, LANES), bf16),
                pltpu.VMEM((R + plan.half, LANES), bf16),
                pltpu.VMEM((R + plan.half, LANES), bf16),
                dma((3,)),
                dma((5,)),
                dma((3, N - 1)),
                dma((2,)),
                dma((2,)),
                dma((G // 2, B)),
                dma((B - 1,)),
                dma((G // 2, B)),
                dma((2, B - 1)),
                dma((2, B - 1)),
                dma((G // 2,)),
                dma((G // 2,)),
                dma((2, 2)),
            ],
            compiler_params=pltpu.CompilerParams(
                collective_id=0, has_side_effects=True, vmem_limit_bytes=60 * 1024 * 1024
            ),
        )(queries, keys, values, valid.reshape(1, rows), offsets)
        return pl.pallas_call(
            functools.partial(project, plan),
            out_shape=jax.ShapeDtypeStruct((rows, w_out.shape[1]), bf16),
            in_specs=[vmem] * 4,
            out_specs=vmem,
            compiler_params=pltpu.CompilerParams(vmem_limit_bytes=8 * 1024 * 1024),
        )(*attended, w_out)

    rows_spec = P(("grp", "blk", "set"), None)
    return jax.shard_map(
        per_device,
        mesh=mesh,
        in_specs=(rows_spec, rows_spec, rows_spec, P(("grp", "blk", "set")), P(), P()),
        out_specs=rows_spec,
        check_vma=False,
    )
```

```python
import functools

import jax
import jax.numpy as jnp
from jax import lax
from jax.experimental import pallas as pl
from jax.experimental.pallas import tpu as pltpu
from jax.sharding import PartitionSpec as P

HEAD_COUNT = 6
HD = 64
LANES = 128
UNIT = 16
FLAG_STRIDE = 8
CHUNKS = HEAD_COUNT * HD // LANES
SETS = ((0, 3, 4), (2, 1, 5))
PARTS = 3
MESH = pl.DeviceIdType.MESH
NEG = -1e30


def units(count):
    return -(-count // UNIT)


def split_pow2(x, size):
    shift = size.bit_length() - 1
    return lax.shift_right_logical(x, shift), x & (size - 1)


class Plan:
    def __init__(self, grp, blk, n, rows):
        self.grp, self.blk, self.n, self.rows = grp, blk, n, rows
        self.period = grp * blk
        self.c3 = rows // self.period
        c2 = rows // blk
        self.counts = (self.c3, c2 - self.c3, rows - c2)
        self.units = tuple(units(c) for c in self.counts)
        self.sizes = tuple(u * UNIT for u in self.units)
        self.starts = (0, self.sizes[0], self.sizes[0] + self.sizes[1])
        self.total = sum(self.sizes)
        self.half = units(-(-self.total // 2)) * UNIT

    def source(self, t):
        a = t
        b = t - self.starts[1]
        c = t - self.starts[2]
        bv, bg = split_pow2(b, self.c3)
        cv, cg = split_pow2(c, self.c3)
        ck, cm = split_pow2(cv, self.grp)
        is_a = t < self.starts[1]
        is_b = t < self.starts[2]
        group = jnp.where(is_a, a, jnp.where(is_b, bg, cg))
        slot = jnp.where(is_a, 0, jnp.where(is_b, (bv + 1) * self.blk, cm * self.blk + ck + 1))
        local = jnp.where(is_a, a, jnp.where(is_b, b, c))
        count = jnp.where(is_a, self.counts[0], jnp.where(is_b, self.counts[1], self.counts[2]))
        return jnp.where(local < count, group * self.period, -(1 << 20)), slot


def flip(s, r):
    step = 1
    while step <= r:
        if r & step:
            s = s + step * (1 - 2 * ((s // step) % 2))
        step *= 2
    return s


def unfold(plan, x):
    x = x.astype(jnp.float32)
    low = pltpu.roll(x, HD, 1)[:plan.total - plan.half]
    return jnp.concatenate([x, low], axis=0).astype(jnp.bfloat16)


def kernel(
    plan, q_hbm, k_hbm, v_hbm, valid_hbm, offs_hbm, own_o, ret_r, back_hot,
    qkv_ref, valid_ref, offs_ref,
    buf_a, buf_b, buf_c, snd_a, snd_b, snd_c, snd_q, own_q, got_q, ret_s,
    load, zsend, zrecv, crecv, qsem, asend, afirst, arecv, bsend, brecv, fsend, frecv, rsem,
):
    G, B, N = plan.grp, plan.blk, plan.n
    R = plan.total
    K = G // 2
    H = plan.half
    gi, bi, si = lax.axis_index("grp"), lax.axis_index("blk"), lax.axis_index("set")
    core = gi % 2
    partner = gi + 1 - 2 * core
    even = si % 2 == 0

    def peer(sx, sy):
        return (lax.rem(gi + 2 * sx, G), lax.rem(bi + sy, B), si)


    across = [(x, y) for x in range(K) for y in range(B) if x or y]
    near = [(x, y) for x, y in across if not (x and y)]
    diagonal = [(x, y) for x, y in across if x and y]

    barrier = pltpu.get_barrier_semaphore()

    def greet(device):
        pl.semaphore_signal(barrier, inc=1, device_id=device, device_id_type=MESH)

    for r in range(N - 1, 0, -1):
        greet((gi, bi, flip(si, r)))
    for x, y in near:
        greet(peer(x, y))
    greet((partner, bi, si))

    load_offs = pltpu.make_async_copy(offs_hbm, offs_ref, load.at[0])
    load_valid = pltpu.make_async_copy(valid_hbm, valid_ref, load.at[1])
    load_qkv = [pltpu.make_async_copy(src, qkv_ref.at[n], load.at[2]) for n, src in enumerate((q_hbm, k_hbm, v_hbm))]
    for copy in (load_offs, load_valid, *load_qkv):
        copy.start()
    load_offs.wait()
    load_valid.wait()
    pltpu.make_async_copy(qkv_ref, qkv_ref, load.at[2]).wait()

    lane = lax.broadcasted_iota(jnp.int32, (R, LANES), 1)
    left = lane < HD
    base, slot = plan.source(lax.broadcasted_iota(jnp.int32, (R, plan.rows), 0))
    token = lax.broadcasted_iota(jnp.int32, (R, plan.rows), 1)
    valid_row = (valid_ref[...] > 0).astype(jnp.float32)
    flag_lane = lax.broadcasted_iota(jnp.int32, (UNIT, LANES), 1)

    moved = {}
    columns = {}
    for h in range(HEAD_COUNT):
        cols = slice((h // 2) * LANES, (h // 2 + 1) * LANES)
        packed = jnp.concatenate([qkv_ref[n, :, cols] for n in range(3)], axis=1)
        hit = token == base + ((slot + offs_ref[1, h]) & (plan.period - 1))
        onehot = jnp.where(hit, jnp.float32(1), jnp.float32(0))
        moved[h] = jnp.dot(onehot.astype(jnp.bfloat16), packed, preferred_element_type=jnp.float32)
        columns[h] = jnp.sum(onehot * valid_row, axis=1, keepdims=True)

    def piece(h, which):
        return moved[h][:, which * LANES:(which + 1) * LANES]

    def fold(x, keep):
        low = x[H:]
        if R < 2 * H:
            low = jnp.concatenate([low, jnp.zeros((2 * H - R, LANES), low.dtype)], axis=0)
        return jnp.where(keep, x[:H], pltpu.roll(low, HD, 1))

    packs = []
    for number, (a, b, c) in enumerate(SETS):
        flags = jnp.zeros((UNIT, LANES), jnp.float32)
        for j, h in enumerate((a, b, c)):
            for u in range(R // UNIT):
                flags = jnp.where(
                    flag_lane == u * FLAG_STRIDE + j, columns[h][u * UNIT:(u + 1) * UNIT, :], flags
                )
        turned = pltpu.roll(piece(c, 2), HD, 1)
        mixed = jnp.where(left, piece(c, 1), turned) if number == 0 else jnp.where(left, turned, piece(c, 1))
        packs.append(
            (
                jnp.where(left, piece(a, 1), piece(b, 1)),
                jnp.where(left, piece(a, 2), piece(b, 2)),
                mixed,
                jnp.where(left, piece(a, 0), piece(b, 0)) * 0.125,
                piece(c, 0) * 0.125,
                flags,
                fold(piece(c, 0) * 0.125, left[:H] if number == 0 else ~left[:H]),
            )
        )
    mine = [jnp.where(even, x, y).astype(jnp.bfloat16) for x, y in zip(*packs)]
    other = [jnp.where(even, y, x).astype(jnp.bfloat16) for x, y in zip(*packs)]
    a_end, b_end = plan.starts[1], plan.starts[2]
    for j in range(PARTS):
        buf_a[0, 0, 0, j] = mine[j][:a_end]
        snd_a[j] = other[j][:a_end]
        buf_b[0, 0, j] = mine[j][a_end:b_end]
        snd_b[j] = other[j][a_end:b_end]
        buf_c[0, j] = mine[j][b_end:]
        snd_c[j] = other[j][b_end:]
    buf_a[0, 0, 0, PARTS, 0:UNIT] = mine[5]
    snd_a[PARTS, 0:UNIT] = other[5]
    for j in range(2):
        own_q[j] = mine[3 + j]
    snd_q[0:R] = other[3]
    snd_q[R:R + H] = other[6]

    pl.semaphore_wait(barrier, (N - 1) + len(near) + 1)

    heads = (slice(0, 2), slice(2, 3))
    line_sem = (lambda r: zrecv.at[0, r - 1], lambda r: zrecv.at[1, r - 1], lambda r: zrecv.at[2, r - 1])

    def line_ref(part, r):
        if part == 0:
            return buf_a.at[0, 0, r]
        if part < 3:
            return buf_b.at[0, r, heads[part - 1]]
        return buf_c.at[r, heads[part - 3]]

    def zcopy(part, r):
        sent = snd_a if part == 0 else (snd_b if part < 3 else snd_c).at[heads[(part - 1) % 2]]
        return pltpu.make_async_remote_copy(
            src_ref=sent if r % 2 else line_ref(part, 0),
            dst_ref=line_ref(part, r),
            send_sem=zsend.at[part],
            recv_sem=line_sem[part](r) if part < 3 else crecv.at[part - 3],
            device_id=(gi, bi, flip(si, r)), device_id_type=MESH,
        )

    def line_sent(part):
        rest = slice(1, N)
        ref = (
            buf_a.at[0, 0, rest] if part == 0
            else buf_b.at[0, rest, heads[part - 1]] if part < 3
            else buf_c.at[rest, heads[part - 3]]
        )
        pltpu.make_async_copy(ref, ref, zsend.at[part]).wait()

    def qcopy():
        return pltpu.make_async_remote_copy(
            src_ref=snd_q, dst_ref=got_q, send_sem=qsem.at[0], recv_sem=qsem.at[1],
            device_id=(gi, bi, flip(si, 1)), device_id_type=MESH,
        )

    def acopy(x, y, r):
        return pltpu.make_async_remote_copy(
            src_ref=buf_a.at[0, 0, r], dst_ref=buf_a.at[2 * x, y, r],
            send_sem=asend.at[x, y],
            recv_sem=afirst.at[y - 1] if x == 0 and r == 0 else arecv.at[x, y],
            device_id=peer((K - x) % K, (B - y) % B), device_id_type=MESH,
        )

    def bcopy(y, r, j):
        return pltpu.make_async_remote_copy(
            src_ref=buf_b.at[0, r, heads[j]], dst_ref=buf_b.at[y, r, heads[j]],
            send_sem=bsend.at[j, y - 1], recv_sem=brecv.at[j, y - 1],
            device_id=peer(0, B - y), device_id_type=MESH,
        )

    def fcopy(x, y):
        return pltpu.make_async_remote_copy(
            src_ref=buf_a.at[2 * x, y], dst_ref=buf_a.at[2 * x + 1, y],
            send_sem=fsend.at[x], recv_sem=frecv.at[x],
            device_id=(partner, bi, si), device_id_type=MESH,
        )

    def rcopy(j):
        rows = (slice(0, R), slice(R, R + H))[j]
        return pltpu.make_async_remote_copy(
            src_ref=ret_s.at[rows], dst_ref=ret_r.at[rows], send_sem=rsem.at[0, j], recv_sem=rsem.at[1, j],
            device_id=(gi, bi, flip(si, 1)), device_id_type=MESH,
        )

    def arrived(ref, sem):
        pltpu.make_async_copy(ref, ref, sem).wait()

    def spread_a(r, where):
        for x, y in where:
            acopy(x, y, r).start()

    def spread_b(r, j):
        for y in range(1, B):
            bcopy(y, r, j).start()

    order = list(range(N - 1, 0, -1))

    def send_line(part):
        for r in order:
            zcopy(part, r).start()

    send_line(0)
    spread_a(0, near)
    send_line(1)
    spread_b(0, 0)
    send_line(2)
    spread_b(0, 1)

    token = lax.broadcasted_iota(jnp.int32, (plan.rows, R), 0)
    base, slot = plan.source(lax.broadcasted_iota(jnp.int32, (plan.rows, R), 1))
    for h in range(HEAD_COUNT):
        hit = token == base + ((slot + offs_ref[1, h]) & (plan.period - 1))
        back_hot[h] = jnp.where(hit, jnp.float32(1), jnp.float32(0)).astype(jnp.bfloat16)

    for y in range(1, B):
        acopy(0, y, 0).wait_recv()
    spread_a(0, diagonal)
    for r in range(1, N):
        zcopy(0, r).wait_recv()
        spread_a(r, across)
    fcopy(0, 0).start()
    qcopy().start()
    send_line(3)
    send_line(4)
    for r in range(1, N):
        zcopy(1, r).wait_recv()
        spread_b(r, 0)
    for r in range(1, N):
        zcopy(2, r).wait_recv()
        spread_b(r, 1)
    for x, y in across:
        arrived(buf_a.at[2 * x, y] if x else buf_a.at[0, y, 1:N], arecv.at[x, y])
        fcopy(x, y).start()

    head_pick = lax.broadcasted_iota(jnp.int32, (FLAG_STRIDE, LANES), 1) & (FLAG_STRIDE - 1)
    head_pick = head_pick == lax.broadcasted_iota(jnp.int32, (FLAG_STRIDE, LANES), 0)
    head_pick = jnp.where(head_pick, jnp.float32(1), jnp.float32(0)).astype(jnp.bfloat16)

    def gather(level, at):
        pieces = []
        for u in range(plan.units[0]):
            rows = slice(u * UNIT, (u + 1) * UNIT)
            part = (buf_a[0, 0, :, at, rows], buf_a[0, :, :, at, rows], buf_a[:, :, :, at, rows])[level]
            pieces.append(part.reshape(-1, LANES))
        if level < 2:
            for u in range(plan.units[1]):
                rows = slice(u * UNIT, (u + 1) * UNIT)
                part = buf_b[0, :, at, rows] if level == 0 else buf_b[:, :, at, rows]
                pieces.append(part.reshape(-1, LANES))
        if level == 0:
            for u in range(plan.units[2]):
                pieces.append(buf_c[:, at, u * UNIT:(u + 1) * UNIT].reshape(-1, LANES))
        return pieces[0] if len(pieces) == 1 else jnp.concatenate(pieces, axis=0)

    def level_attend(level):
        M = (R, b_end, a_end)[level]
        tiles = M // UNIT
        devices = (N, B * N, G * B * N)[level]
        per_unit = devices * UNIT
        rows = slice(0, UNIT)
        at = PARTS
        tall = (buf_a[0, 0, :, at, rows], buf_a[0, :, :, at, rows], buf_a[:, :, :, at, rows])[level]
        tall = tall.reshape(per_unit, LANES).astype(jnp.float32)
        unit_lane = lax.broadcasted_iota(jnp.int32, (per_unit, LANES), 1) // FLAG_STRIDE
        tall = [jnp.where(unit_lane == u, tall, 0.0).astype(jnp.bfloat16) for u in range(tiles)]
        tall = tall[0] if tiles == 1 else jnp.concatenate(tall, axis=0)
        ok = lax.dot_general(
            head_pick, tall, (((1,), (1,)), ((), ())), preferred_element_type=jnp.float32
        )
        keys = per_unit * tiles
        diagonal_tile = lax.broadcasted_iota(jnp.int32, (UNIT, LANES), 1) - lax.broadcasted_iota(
            jnp.int32, (UNIT, LANES), 0
        )

        def allow(s, bias):
            masked = s + bias
            rows = []
            for who in range(2):
                for u in range(tiles):
                    at = slice((who * tiles + u) * UNIT, (who * tiles + u + 1) * UNIT)
                    spot = u * per_unit + who * UNIT
                    tile = slice(spot // LANES * LANES, spot // LANES * LANES + LANES)
                    fixed = jnp.where(diagonal_tile == spot % LANES, s[at, tile], masked[at, tile])
                    pieces = [masked[at, :tile.start], fixed, masked[at, tile.stop:]]
                    rows.append(jnp.concatenate([p for p in pieces if p.shape[1]], axis=1))
            return jnp.concatenate(rows, axis=0)

        bias = jnp.where(ok > 0.5, 0.0, NEG)
        half_lane = lax.broadcasted_iota(jnp.int32, (2 * M, LANES), 1) < HD
        value_lane = half_lane != even
        contract = (((1,), (1,)), ((), ()))
        zero = jnp.zeros((2 * M, LANES), jnp.bfloat16)

        def query(j):
            return jnp.concatenate([own_q[j, 0:M], got_q[0:M] if j == 0 else got_single[0:M]], axis=0)

        def scores(part):
            q = query(part)
            keys = gather(level, 2 * part)
            if part == 0:
                q = jnp.concatenate([jnp.where(half_lane, q, zero), jnp.where(half_lane, zero, q)], axis=0)
            else:
                q = jnp.where(value_lane, zero, q)
            s = lax.dot_general(q, keys, contract, preferred_element_type=jnp.float32)
            return [s[:2 * M], s[2 * M:]] if part == 0 else [s]

        def masked(s, part):
            return [allow(x, bias[2 * part + n:2 * part + n + 1, :]) for n, x in enumerate(s)]

        def mix(probs, part):
            values = gather(level, 1 + part)
            return jnp.dot(jnp.concatenate(probs, axis=0), values, preferred_element_type=jnp.float32)

        def finish(mixed, totals, lses, part):
            if part == 1:
                return mixed / totals[0], jnp.broadcast_to(lses[0], (2 * M, LANES))
            return (
                jnp.where(half_lane, mixed[:2 * M] / totals[0], mixed[2 * M:] / totals[1]),
                jnp.where(half_lane, lses[0], lses[1]),
            )

        return scores, masked, mix, finish

    def attend(jobs):
        scores = [level[0](part) for level, part in jobs]
        scores = [level[1](s, part) for s, (level, part) in zip(scores, jobs)]
        tops = [[jnp.max(x, axis=1, keepdims=True) for x in s] for s in scores]
        weights = [[jnp.exp(x - t) for x, t in zip(s, top)] for s, top in zip(scores, tops)]
        probs = [[x.astype(jnp.bfloat16) for x in w] for w in weights]
        mixed = [level[2](p, part) for p, (level, part) in zip(probs, jobs)]
        totals = [[jnp.sum(x, axis=1, keepdims=True) for x in w] for w in weights]
        lses = [[t + jnp.log(x) for t, x in zip(top, total)] for top, total in zip(tops, totals)]
        return [
            level[3](m, total, lse, part) for m, total, lse, (level, part) in zip(mixed, totals, lses, jobs)
        ]

    def combine(levels):
        top = functools.reduce(jnp.maximum, [lse for _, lse in levels])
        shares = [jnp.exp(lse - top) for _, lse in levels]
        return sum(s * o for s, (o, _) in zip(shares, levels)) / sum(shares)

    qcopy().wait_recv()
    for x in range(K):
        arrived(buf_a.at[2 * x + 1], frecv.at[x])
    got_single = unfold(plan, got_q[R:R + H])
    outer, middle, dense = level_attend(2), level_attend(1), level_attend(0)
    value_half = left[:H] != even
    for j in range(2):
        for y in range(1, B):
            arrived(buf_b.at[y, :, heads[j]], brecv.at[j, y - 1])
        arrived(buf_c.at[1:N, heads[j]], crecv.at[j])
        jobs = [(middle, j), (dense, j)]
        if j == 0:
            second, first, *third = attend(jobs + [(outer, 0), (outer, 1)])
        else:
            second, first = attend(jobs)
        for who in (1, 0):
            (o1, l1), (o2, l2), (o3, l3) = [
                tuple(x[who * m:(who + 1) * m] for x in level)
                for level, m in ((first, R), (second, b_end), (third[j], a_end))
            ]
            mixed = jnp.concatenate(
                [
                    combine([(o1[:a_end], l1[:a_end]), (o2[:a_end], l2[:a_end]), (o3, l3)]),
                    combine([(o1[a_end:b_end], l1[a_end:b_end]), (o2[a_end:], l2[a_end:])]),
                    o1[b_end:],
                ],
                axis=0,
            )
            if who == 0:
                own_o[j] = mixed.astype(jnp.bfloat16)
            else:
                if j == 0:
                    ret_s[0:R] = mixed.astype(jnp.bfloat16)
                else:
                    ret_s[R:R + H] = fold(mixed, value_half).astype(jnp.bfloat16)
                rcopy(j).start()
    for part in range(5):
        line_sent(part)
    qcopy().wait_send()
    for x, y in across:
        arrived(buf_a.at[0, 0], asend.at[x, y])
    for j in range(2):
        for y in range(1, B):
            arrived(buf_b.at[0, :, heads[j]], bsend.at[j, y - 1])
    for x in range(K):
        arrived(buf_a.at[2 * x], fsend.at[x])
    for j in range(2):
        rcopy(j).wait_recv()

    for j in range(2):
        rcopy(j).wait_send()


def project(plan, own_o, ret_r, back_hot, w_ref, o_ref):
    R, H = plan.total, plan.half
    even = lax.axis_index("set") % 2 == 0
    left = lax.broadcasted_iota(jnp.int32, (R, LANES), 1) < HD
    got = (ret_r[0:R], unfold(plan, ret_r[R:R + H]))
    sets = [
        (jnp.where(even, own_o[j], got[j]), jnp.where(even, got[j], own_o[j])) for j in range(2)
    ]
    (zero_pair, one_pair), (zero_single, one_single) = sets
    singles = jnp.where(left, one_single, zero_single)
    out_left = lax.broadcasted_iota(jnp.int32, (plan.rows, LANES), 1) < HD
    attention, weights = [], []
    for value, (a, b) in ((zero_pair, SETS[0][:2]), (one_pair, SETS[1][:2]), (singles, (SETS[1][2], SETS[0][2]))):
        back = [jnp.dot(back_hot[h], value, preferred_element_type=jnp.float32) for h in (a, b)]
        attention.append(jnp.where(out_left, back[0], back[1]).astype(jnp.bfloat16))
        weights += [w_ref[a * HD:(a + 1) * HD, :], w_ref[b * HD:(b + 1) * HD, :]]
    attention = jnp.concatenate(attention, axis=1)
    weights = jnp.concatenate(weights, axis=0)
    o_ref[...] = jnp.dot(attention, weights, preferred_element_type=jnp.float32).astype(o_ref.dtype)


def solution(mesh):
    G, B, N = mesh.shape["grp"], mesh.shape["blk"], mesh.shape["set"]

    def per_device(queries, keys, values, valid, offsets, w_out):
        rows, width = queries.shape
        plan = Plan(G, B, N, rows)
        vmem = pl.BlockSpec(memory_space=pltpu.VMEM)
        anywhere = pl.BlockSpec(memory_space=pl.ANY)
        dma = pltpu.SemaphoreType.DMA
        ra, rb, rc = plan.sizes
        R = plan.total
        bf16 = jnp.bfloat16
        outputs = ((2, R, LANES), (R + plan.half, LANES), (HEAD_COUNT, rows, R))
        attended = pl.pallas_call(
            functools.partial(kernel, plan),
            out_shape=[pltpu.VMEM(shape, bf16) for shape in outputs],
            in_specs=[anywhere] * 5,
            out_specs=[vmem] * 3,
            cost_estimate=pl.CostEstimate(
                flops=4 * rows * rows * N * width * 4, bytes_accessed=4 * rows * width * 2, transcendentals=0
            ),
            scratch_shapes=[
                pltpu.VMEM((3, rows, width), bf16),
                pltpu.VMEM((1, rows), jnp.int32),
                pltpu.SMEM(offsets.shape, jnp.int32),
                pltpu.VMEM((G, B, N, PARTS + 1, ra, LANES), bf16),
                pltpu.VMEM((B, N, PARTS, rb, LANES), bf16),
                pltpu.VMEM((N, PARTS, rc, LANES), bf16),
                pltpu.VMEM((PARTS + 1, ra, LANES), bf16),
                pltpu.VMEM((PARTS, rb, LANES), bf16),
                pltpu.VMEM((PARTS, rc, LANES), bf16),
                pltpu.VMEM((R + plan.half, LANES), bf16),
                pltpu.VMEM((2, R, LANES), bf16),
                pltpu.VMEM((R + plan.half, LANES), bf16),
                pltpu.VMEM((R + plan.half, LANES), bf16),
                dma((3,)),
                dma((5,)),
                dma((3, N - 1)),
                dma((2,)),
                dma((2,)),
                dma((G // 2, B)),
                dma((B - 1,)),
                dma((G // 2, B)),
                dma((2, B - 1)),
                dma((2, B - 1)),
                dma((G // 2,)),
                dma((G // 2,)),
                dma((2, 2)),
            ],
            compiler_params=pltpu.CompilerParams(
                collective_id=0, has_side_effects=True, vmem_limit_bytes=60 * 1024 * 1024
            ),
        )(queries, keys, values, valid.reshape(1, rows), offsets)
        return pl.pallas_call(
            functools.partial(project, plan),
            out_shape=jax.ShapeDtypeStruct((rows, w_out.shape[1]), bf16),
            in_specs=[vmem] * 4,
            out_specs=vmem,
            compiler_params=pltpu.CompilerParams(vmem_limit_bytes=8 * 1024 * 1024),
        )(*attended, w_out)

    rows_spec = P(("grp", "blk", "set"), None)
    return jax.shard_map(
        per_device,
        mesh=mesh,
        in_specs=(rows_spec, rows_spec, rows_spec, P(("grp", "blk", "set")), P(), P()),
        out_specs=rows_spec,
        check_vma=False,
    )
```

```python
import functools

import jax
import jax.numpy as jnp
from jax import lax
from jax.experimental import pallas as pl
from jax.experimental.pallas import tpu as pltpu
from jax.sharding import PartitionSpec as P

HEAD_COUNT = 6
HD = 64
LANES = 128
UNIT = 16
FLAG_STRIDE = 8
CHUNKS = HEAD_COUNT * HD // LANES
SETS = ((0, 3, 4), (2, 1, 5))
PARTS = 3
MESH = pl.DeviceIdType.MESH
NEG = -1e30


def units(count):
    return -(-count // UNIT)


def split_pow2(x, size):
    shift = size.bit_length() - 1
    return lax.shift_right_logical(x, shift), x & (size - 1)


class Plan:
    def __init__(self, grp, blk, n, rows):
        self.grp, self.blk, self.n, self.rows = grp, blk, n, rows
        self.period = grp * blk
        self.c3 = rows // self.period
        c2 = rows // blk
        self.counts = (self.c3, c2 - self.c3, rows - c2)
        self.units = tuple(units(c) for c in self.counts)
        self.sizes = tuple(u * UNIT for u in self.units)
        self.starts = (0, self.sizes[0], self.sizes[0] + self.sizes[1])
        self.total = sum(self.sizes)
        self.half = units(-(-self.total // 2)) * UNIT

    def source(self, t):
        a = t
        b = t - self.starts[1]
        c = t - self.starts[2]
        bv, bg = split_pow2(b, self.c3)
        cv, cg = split_pow2(c, self.c3)
        ck, cm = split_pow2(cv, self.grp)
        is_a = t < self.starts[1]
        is_b = t < self.starts[2]
        group = jnp.where(is_a, a, jnp.where(is_b, bg, cg))
        slot = jnp.where(is_a, 0, jnp.where(is_b, (bv + 1) * self.blk, cm * self.blk + ck + 1))
        local = jnp.where(is_a, a, jnp.where(is_b, b, c))
        count = jnp.where(is_a, self.counts[0], jnp.where(is_b, self.counts[1], self.counts[2]))
        return jnp.where(local < count, group * self.period, -(1 << 20)), slot


def flip(s, r):
    step = 1
    while step <= r:
        if r & step:
            s = s + step * (1 - 2 * ((s // step) % 2))
        step *= 2
    return s


def unfold(plan, x):
    x = x.astype(jnp.float32)
    low = pltpu.roll(x, HD, 1)[:plan.total - plan.half]
    return jnp.concatenate([x, low], axis=0).astype(jnp.bfloat16)


def kernel(
    plan, q_hbm, k_hbm, v_hbm, valid_hbm, offs_hbm, own_o, ret_r, back_hot,
    qkv_ref, valid_ref, offs_ref,
    buf_a, buf_b, buf_c, snd_a, snd_b, snd_c, snd_q, own_q, got_q, ret_s,
    load, zsend, zrecv, crecv, qsem, asend, afirst, arecv, bsend, brecv, fsend, frecv, rsem,
):
    G, B, N = plan.grp, plan.blk, plan.n
    R = plan.total
    K = G // 2
    H = plan.half
    gi, bi, si = lax.axis_index("grp"), lax.axis_index("blk"), lax.axis_index("set")
    core = gi % 2
    partner = gi + 1 - 2 * core
    even = si % 2 == 0

    def peer(sx, sy):
        return (lax.rem(gi + 2 * sx, G), lax.rem(bi + sy, B), si)


    load_offs = pltpu.make_async_copy(offs_hbm, offs_ref, load.at[0])
    load_valid = pltpu.make_async_copy(valid_hbm, valid_ref, load.at[1])
    load_qkv = [pltpu.make_async_copy(src, qkv_ref.at[n], load.at[2]) for n, src in enumerate((q_hbm, k_hbm, v_hbm))]
    for copy in (*load_qkv, load_offs, load_valid):
        copy.start()

    across = [(x, y) for x in range(K) for y in range(B) if x or y]
    near = [(x, y) for x, y in across if not (x and y)]
    diagonal = [(x, y) for x, y in across if x and y]

    barrier = pltpu.get_barrier_semaphore()

    def greet(device):
        pl.semaphore_signal(barrier, inc=1, device_id=device, device_id_type=MESH)

    for r in range(N - 1, 0, -1):
        greet((gi, bi, flip(si, r)))
    for x, y in near:
        greet(peer(x, y))
    greet((partner, bi, si))

    load_offs.wait()
    load_valid.wait()
    pltpu.make_async_copy(qkv_ref, qkv_ref, load.at[2]).wait()

    lane = lax.broadcasted_iota(jnp.int32, (R, LANES), 1)
    left = lane < HD
    base, slot = plan.source(lax.broadcasted_iota(jnp.int32, (R, plan.rows), 0))
    token = lax.broadcasted_iota(jnp.int32, (R, plan.rows), 1)
    valid_row = (valid_ref[...] > 0).astype(jnp.float32)
    flag_lane = lax.broadcasted_iota(jnp.int32, (UNIT, LANES), 1)

    moved = {}
    columns = {}
    for c in range(CHUNKS):
        cols = slice(c * LANES, (c + 1) * LANES)
        packed = jnp.concatenate([qkv_ref[n, :, cols] for n in range(3)], axis=1)
        hits = []
        for h in (2 * c, 2 * c + 1):
            hit = token == base + ((slot + offs_ref[1, h]) & (plan.period - 1))
            onehot = jnp.where(hit, jnp.float32(1), jnp.float32(0))
            columns[h] = jnp.sum(onehot * valid_row, axis=1, keepdims=True)
            hits.append(onehot.astype(jnp.bfloat16))
        both = jnp.dot(jnp.concatenate(hits, axis=0), packed, preferred_element_type=jnp.float32)
        moved[2 * c], moved[2 * c + 1] = both[:R], both[R:]

    def piece(h, which):
        return moved[h][:, which * LANES:(which + 1) * LANES]

    def fold(x, keep):
        low = x[H:]
        if R < 2 * H:
            low = jnp.concatenate([low, jnp.zeros((2 * H - R, LANES), low.dtype)], axis=0)
        return jnp.where(keep, x[:H], pltpu.roll(low, HD, 1))

    packs = []
    for number, (a, b, c) in enumerate(SETS):
        flags = jnp.zeros((UNIT, LANES), jnp.float32)
        for j, h in enumerate((a, b, c)):
            for u in range(R // UNIT):
                flags = jnp.where(
                    flag_lane == u * FLAG_STRIDE + j, columns[h][u * UNIT:(u + 1) * UNIT, :], flags
                )
        turned = pltpu.roll(piece(c, 2), HD, 1)
        mixed = jnp.where(left, piece(c, 1), turned) if number == 0 else jnp.where(left, turned, piece(c, 1))
        packs.append(
            (
                jnp.where(left, piece(a, 1), piece(b, 1)),
                jnp.where(left, piece(a, 2), piece(b, 2)),
                mixed,
                jnp.where(left, piece(a, 0), piece(b, 0)) * 0.125,
                piece(c, 0) * 0.125,
                flags,
                fold(piece(c, 0) * 0.125, left[:H] if number == 0 else ~left[:H]),
            )
        )
    mine = [jnp.where(even, x, y).astype(jnp.bfloat16) for x, y in zip(*packs)]
    other = [jnp.where(even, y, x).astype(jnp.bfloat16) for x, y in zip(*packs)]
    a_end, b_end = plan.starts[1], plan.starts[2]
    for j in range(PARTS):
        buf_a[0, 0, 0, j] = mine[j][:a_end]
        snd_a[j] = other[j][:a_end]
        buf_b[0, 0, j] = mine[j][a_end:b_end]
        snd_b[j] = other[j][a_end:b_end]
        buf_c[0, j] = mine[j][b_end:]
        snd_c[j] = other[j][b_end:]
    buf_a[0, 0, 0, PARTS, 0:UNIT] = mine[5]
    snd_a[PARTS, 0:UNIT] = other[5]
    for j in range(2):
        own_q[j] = mine[3 + j]
    snd_q[0:R] = other[3]
    snd_q[R:R + H] = other[6]

    pl.semaphore_wait(barrier, (N - 1) + len(near) + 1)

    heads = (slice(0, 2), slice(2, 3))
    line_sem = (lambda r: zrecv.at[0, r - 1], lambda r: zrecv.at[1, r - 1], lambda r: zrecv.at[2, r - 1])

    def line_ref(part, r):
        if part == 0:
            return buf_a.at[0, 0, r]
        if part < 3:
            return buf_b.at[0, r, heads[part - 1]]
        return buf_c.at[r, heads[part - 3]]

    def zcopy(part, r):
        sent = snd_a if part == 0 else (snd_b if part < 3 else snd_c).at[heads[(part - 1) % 2]]
        return pltpu.make_async_remote_copy(
            src_ref=sent if r % 2 else line_ref(part, 0),
            dst_ref=line_ref(part, r),
            send_sem=zsend.at[part],
            recv_sem=line_sem[part](r) if part < 3 else crecv.at[part - 3],
            device_id=(gi, bi, flip(si, r)), device_id_type=MESH,
        )

    def line_sent(part):
        rest = slice(1, N)
        ref = (
            buf_a.at[0, 0, rest] if part == 0
            else buf_b.at[0, rest, heads[part - 1]] if part < 3
            else buf_c.at[rest, heads[part - 3]]
        )
        pltpu.make_async_copy(ref, ref, zsend.at[part]).wait()

    def qcopy():
        return pltpu.make_async_remote_copy(
            src_ref=snd_q, dst_ref=got_q, send_sem=qsem.at[0], recv_sem=qsem.at[1],
            device_id=(gi, bi, flip(si, 1)), device_id_type=MESH,
        )

    def acopy(x, y, r):
        return pltpu.make_async_remote_copy(
            src_ref=buf_a.at[0, 0, r], dst_ref=buf_a.at[2 * x, y, r],
            send_sem=asend.at[x, y],
            recv_sem=afirst.at[y - 1] if x == 0 and r == 0 else arecv.at[x, y],
            device_id=peer((K - x) % K, (B - y) % B), device_id_type=MESH,
        )

    def bcopy(y, r, j):
        return pltpu.make_async_remote_copy(
            src_ref=buf_b.at[0, r, heads[j]], dst_ref=buf_b.at[y, r, heads[j]],
            send_sem=bsend.at[j, y - 1], recv_sem=brecv.at[j, y - 1],
            device_id=peer(0, B - y), device_id_type=MESH,
        )

    def fcopy(x, y):
        return pltpu.make_async_remote_copy(
            src_ref=buf_a.at[2 * x, y], dst_ref=buf_a.at[2 * x + 1, y],
            send_sem=fsend.at[x], recv_sem=frecv.at[x],
            device_id=(partner, bi, si), device_id_type=MESH,
        )

    def rcopy(j):
        rows = (slice(0, R), slice(R, R + H))[j]
        return pltpu.make_async_remote_copy(
            src_ref=ret_s.at[rows], dst_ref=ret_r.at[rows], send_sem=rsem.at[0, j], recv_sem=rsem.at[1, j],
            device_id=(gi, bi, flip(si, 1)), device_id_type=MESH,
        )

    def arrived(ref, sem):
        pltpu.make_async_copy(ref, ref, sem).wait()

    def spread_a(r, where):
        for x, y in where:
            acopy(x, y, r).start()

    def spread_b(r, j):
        for y in range(1, B):
            bcopy(y, r, j).start()

    order = list(range(N - 1, 0, -1))

    def send_line(part):
        for r in order:
            zcopy(part, r).start()

    send_line(0)
    spread_a(0, near)
    send_line(1)
    spread_b(0, 0)
    send_line(2)
    spread_b(0, 1)

    token = lax.broadcasted_iota(jnp.int32, (plan.rows, R), 0)
    base, slot = plan.source(lax.broadcasted_iota(jnp.int32, (plan.rows, R), 1))
    for h in range(HEAD_COUNT):
        hit = token == base + ((slot + offs_ref[1, h]) & (plan.period - 1))
        back_hot[h] = jnp.where(hit, jnp.float32(1), jnp.float32(0)).astype(jnp.bfloat16)

    for y in range(1, B):
        acopy(0, y, 0).wait_recv()
    spread_a(0, diagonal)
    for r in range(1, N):
        zcopy(0, r).wait_recv()
        spread_a(r, across)
    fcopy(0, 0).start()
    qcopy().start()
    send_line(3)
    send_line(4)
    for r in range(1, N):
        zcopy(1, r).wait_recv()
        spread_b(r, 0)
    for r in range(1, N):
        zcopy(2, r).wait_recv()
        spread_b(r, 1)
    for x, y in across:
        arrived(buf_a.at[2 * x, y] if x else buf_a.at[0, y, 1:N], arecv.at[x, y])
        fcopy(x, y).start()

    head_pick = lax.broadcasted_iota(jnp.int32, (FLAG_STRIDE, LANES), 1) & (FLAG_STRIDE - 1)
    head_pick = head_pick == lax.broadcasted_iota(jnp.int32, (FLAG_STRIDE, LANES), 0)
    head_pick = jnp.where(head_pick, jnp.float32(1), jnp.float32(0)).astype(jnp.bfloat16)

    def gather(level, at):
        pieces = []
        for u in range(plan.units[0]):
            rows = slice(u * UNIT, (u + 1) * UNIT)
            part = (buf_a[0, 0, :, at, rows], buf_a[0, :, :, at, rows], buf_a[:, :, :, at, rows])[level]
            pieces.append(part.reshape(-1, LANES))
        if level < 2:
            for u in range(plan.units[1]):
                rows = slice(u * UNIT, (u + 1) * UNIT)
                part = buf_b[0, :, at, rows] if level == 0 else buf_b[:, :, at, rows]
                pieces.append(part.reshape(-1, LANES))
        if level == 0:
            for u in range(plan.units[2]):
                pieces.append(buf_c[:, at, u * UNIT:(u + 1) * UNIT].reshape(-1, LANES))
        return pieces[0] if len(pieces) == 1 else jnp.concatenate(pieces, axis=0)

    def level_attend(level):
        M = (R, b_end, a_end)[level]
        tiles = M // UNIT
        devices = (N, B * N, G * B * N)[level]
        per_unit = devices * UNIT
        rows = slice(0, UNIT)
        at = PARTS
        tall = (buf_a[0, 0, :, at, rows], buf_a[0, :, :, at, rows], buf_a[:, :, :, at, rows])[level]
        tall = tall.reshape(per_unit, LANES).astype(jnp.float32)
        unit_lane = lax.broadcasted_iota(jnp.int32, (per_unit, LANES), 1) // FLAG_STRIDE
        tall = [jnp.where(unit_lane == u, tall, 0.0).astype(jnp.bfloat16) for u in range(tiles)]
        tall = tall[0] if tiles == 1 else jnp.concatenate(tall, axis=0)
        ok = lax.dot_general(
            head_pick, tall, (((1,), (1,)), ((), ())), preferred_element_type=jnp.float32
        )
        keys = per_unit * tiles
        diagonal_tile = lax.broadcasted_iota(jnp.int32, (UNIT, LANES), 1) - lax.broadcasted_iota(
            jnp.int32, (UNIT, LANES), 0
        )

        def allow(s, bias, who):
            masked = s + bias
            rows = []
            for u in range(tiles):
                at = slice(u * UNIT, (u + 1) * UNIT)
                spot = u * per_unit + who * UNIT
                tile = slice(spot // LANES * LANES, spot // LANES * LANES + LANES)
                fixed = jnp.where(diagonal_tile == spot % LANES, s[at, tile], masked[at, tile])
                pieces = [masked[at, :tile.start], fixed, masked[at, tile.stop:]]
                rows.append(jnp.concatenate([p for p in pieces if p.shape[1]], axis=1))
            return jnp.concatenate(rows, axis=0)

        bias = jnp.where(ok > 0.5, 0.0, NEG)
        half_lane = lax.broadcasted_iota(jnp.int32, (M, LANES), 1) < HD
        value_lane = half_lane != even
        contract = (((1,), (1,)), ((), ()))
        zero = jnp.zeros((M, LANES), jnp.bfloat16)

        def scores(part, who):
            q = own_q[part, 0:M] if who == 0 else got_q[0:M] if part == 0 else got_single[0:M]
            keys = gather(level, 2 * part)
            if part == 0:
                q = jnp.concatenate([jnp.where(half_lane, q, zero), jnp.where(half_lane, zero, q)], axis=0)
            else:
                q = jnp.where(value_lane, zero, q)
            s = lax.dot_general(q, keys, contract, preferred_element_type=jnp.float32)
            return [s[:M], s[M:]] if part == 0 else [s]

        def masked(s, part, who):
            return [allow(x, bias[2 * part + n:2 * part + n + 1, :], who) for n, x in enumerate(s)]

        def mix(probs, part):
            values = gather(level, 1 + part)
            return jnp.dot(jnp.concatenate(probs, axis=0), values, preferred_element_type=jnp.float32)

        def finish(mixed, tops, totals, part):
            if part == 1:
                return (mixed, *(jnp.broadcast_to(x[0], (M, LANES)) for x in (tops, totals)))
            return (
                jnp.where(half_lane, mixed[:M], mixed[M:]),
                *(jnp.where(half_lane, x[0], x[1]) for x in (tops, totals)),
            )

        return scores, masked, mix, finish

    def attend(jobs, who):
        scores = [level[0](part, who) for level, part in jobs]
        scores = [level[1](s, part, who) for s, (level, part) in zip(scores, jobs)]
        tops = [[jnp.max(x, axis=1, keepdims=True) for x in s] for s in scores]
        weights = [[jnp.exp(x - t) for x, t in zip(s, top)] for s, top in zip(scores, tops)]
        probs = [[x.astype(jnp.bfloat16) for x in w] for w in weights]
        mixed = [level[2](p, part) for p, (level, part) in zip(probs, jobs)]
        totals = [[jnp.sum(x, axis=1, keepdims=True) for x in w] for w in weights]
        return [
            level[3](m, top, total, part) for m, top, total, (level, part) in zip(mixed, tops, totals, jobs)
        ]

    def combine(*levels):
        highest = functools.reduce(jnp.maximum, [top for _, top, _ in levels])
        shares = [jnp.exp(top - highest) for _, top, _ in levels]
        return sum(s * m for s, (m, _, _) in zip(shares, levels)) / sum(
            s * total for s, (_, _, total) in zip(shares, levels)
        )

    qcopy().wait_recv()
    for x in range(K):
        arrived(buf_a.at[2 * x + 1], frecv.at[x])
    got_single = unfold(plan, got_q[R:R + H])
    outer, middle, dense = level_attend(2), level_attend(1), level_attend(0)
    value_half = left[:H] != even
    for who, j in ((1, 0), (1, 1), (0, 0), (0, 1)):
        if who == 1:
            for y in range(1, B):
                arrived(buf_b.at[y, :, heads[j]], brecv.at[j, y - 1])
            arrived(buf_c.at[1:N, heads[j]], crecv.at[j])
        jobs = [(middle, j), (dense, j)]
        if j == 0:
            second, first, *third = attend(jobs + [(outer, 0), (outer, 1)], who)
        else:
            second, first = attend(jobs, who)

        def rows(level, start, stop):
            return tuple(x[start:stop] for x in level)

        alone = rows(first, b_end, R)
        mixed = jnp.concatenate(
            [
                combine(rows(first, 0, a_end), rows(second, 0, a_end), third[j]),
                combine(rows(first, a_end, b_end), rows(second, a_end, b_end)),
                alone[0] / alone[2],
            ],
            axis=0,
        )
        if who == 0:
            own_o[j] = mixed.astype(jnp.bfloat16)
        else:
            if j == 0:
                ret_s[0:R] = mixed.astype(jnp.bfloat16)
            else:
                ret_s[R:R + H] = fold(mixed, value_half).astype(jnp.bfloat16)
            rcopy(j).start()
    for part in range(5):
        line_sent(part)
    qcopy().wait_send()
    for x, y in across:
        arrived(buf_a.at[0, 0], asend.at[x, y])
    for j in range(2):
        for y in range(1, B):
            arrived(buf_b.at[0, :, heads[j]], bsend.at[j, y - 1])
    for x in range(K):
        arrived(buf_a.at[2 * x], fsend.at[x])
    for j in range(2):
        rcopy(j).wait_recv()

    for j in range(2):
        rcopy(j).wait_send()


def project(plan, own_o, ret_r, back_hot, w_ref, o_ref):
    R, H = plan.total, plan.half
    even = lax.axis_index("set") % 2 == 0
    left = lax.broadcasted_iota(jnp.int32, (R, LANES), 1) < HD
    got = (ret_r[0:R], unfold(plan, ret_r[R:R + H]))
    sets = [
        (jnp.where(even, own_o[j], got[j]), jnp.where(even, got[j], own_o[j])) for j in range(2)
    ]
    (zero_pair, one_pair), (zero_single, one_single) = sets
    singles = jnp.where(left, one_single, zero_single)
    out_left = lax.broadcasted_iota(jnp.int32, (plan.rows, LANES), 1) < HD
    attention, weights = [], []
    for value, (a, b) in ((zero_pair, SETS[0][:2]), (one_pair, SETS[1][:2]), (singles, (SETS[1][2], SETS[0][2]))):
        back = [jnp.dot(back_hot[h], value, preferred_element_type=jnp.float32) for h in (a, b)]
        attention.append(jnp.where(out_left, back[0], back[1]).astype(jnp.bfloat16))
        weights += [w_ref[a * HD:(a + 1) * HD, :], w_ref[b * HD:(b + 1) * HD, :]]
    attention = jnp.concatenate(attention, axis=1)
    weights = jnp.concatenate(weights, axis=0)
    o_ref[...] = jnp.dot(attention, weights, preferred_element_type=jnp.float32).astype(o_ref.dtype)


def solution(mesh):
    G, B, N = mesh.shape["grp"], mesh.shape["blk"], mesh.shape["set"]

    def per_device(queries, keys, values, valid, offsets, w_out):
        rows, width = queries.shape
        plan = Plan(G, B, N, rows)
        vmem = pl.BlockSpec(memory_space=pltpu.VMEM)
        anywhere = pl.BlockSpec(memory_space=pl.ANY)
        dma = pltpu.SemaphoreType.DMA
        ra, rb, rc = plan.sizes
        R = plan.total
        bf16 = jnp.bfloat16
        outputs = ((2, R, LANES), (R + plan.half, LANES), (HEAD_COUNT, rows, R))
        attended = pl.pallas_call(
            functools.partial(kernel, plan),
            out_shape=[pltpu.VMEM(shape, bf16) for shape in outputs],
            in_specs=[anywhere] * 5,
            out_specs=[vmem] * 3,
            cost_estimate=pl.CostEstimate(
                flops=4 * rows * rows * N * width * 4, bytes_accessed=4 * rows * width * 2, transcendentals=0
            ),
            scratch_shapes=[
                pltpu.VMEM((3, rows, width), bf16),
                pltpu.VMEM((1, rows), jnp.int32),
                pltpu.SMEM(offsets.shape, jnp.int32),
                pltpu.VMEM((G, B, N, PARTS + 1, ra, LANES), bf16),
                pltpu.VMEM((B, N, PARTS, rb, LANES), bf16),
                pltpu.VMEM((N, PARTS, rc, LANES), bf16),
                pltpu.VMEM((PARTS + 1, ra, LANES), bf16),
                pltpu.VMEM((PARTS, rb, LANES), bf16),
                pltpu.VMEM((PARTS, rc, LANES), bf16),
                pltpu.VMEM((R + plan.half, LANES), bf16),
                pltpu.VMEM((2, R, LANES), bf16),
                pltpu.VMEM((R + plan.half, LANES), bf16),
                pltpu.VMEM((R + plan.half, LANES), bf16),
                dma((3,)),
                dma((5,)),
                dma((3, N - 1)),
                dma((2,)),
                dma((2,)),
                dma((G // 2, B)),
                dma((B - 1,)),
                dma((G // 2, B)),
                dma((2, B - 1)),
                dma((2, B - 1)),
                dma((G // 2,)),
                dma((G // 2,)),
                dma((2, 2)),
            ],
            compiler_params=pltpu.CompilerParams(
                collective_id=0, has_side_effects=True, vmem_limit_bytes=60 * 1024 * 1024
            ),
        )(queries, keys, values, valid.reshape(1, rows), offsets)
        return pl.pallas_call(
            functools.partial(project, plan),
            out_shape=jax.ShapeDtypeStruct((rows, w_out.shape[1]), bf16),
            in_specs=[vmem] * 4,
            out_specs=vmem,
            compiler_params=pltpu.CompilerParams(vmem_limit_bytes=8 * 1024 * 1024),
        )(*attended, w_out)

    rows_spec = P(("grp", "blk", "set"), None)
    return jax.shard_map(
        per_device,
        mesh=mesh,
        in_specs=(rows_spec, rows_spec, rows_spec, P(("grp", "blk", "set")), P(), P()),
        out_specs=rows_spec,
        check_vma=False,
    )
```

```python
import functools

import jax
import jax.numpy as jnp
from jax import lax
from jax.experimental import pallas as pl
from jax.experimental.pallas import tpu as pltpu
from jax.sharding import PartitionSpec as P

HEAD_COUNT = 6
HD = 64
LANES = 128
UNIT = 16
FLAG_STRIDE = 8
CHUNKS = HEAD_COUNT * HD // LANES
SETS = ((0, 3, 4), (2, 1, 5))
PARTS = 3
MESH = pl.DeviceIdType.MESH
NEG = -1e30


def units(count):
    return -(-count // UNIT)


def split_pow2(x, size):
    shift = size.bit_length() - 1
    return lax.shift_right_logical(x, shift), x & (size - 1)


class Plan:
    def __init__(self, grp, blk, n, rows):
        self.grp, self.blk, self.n, self.rows = grp, blk, n, rows
        self.period = grp * blk
        self.c3 = rows // self.period
        c2 = rows // blk
        self.counts = (self.c3, c2 - self.c3, rows - c2)
        self.units = tuple(units(c) for c in self.counts)
        self.sizes = tuple(u * UNIT for u in self.units)
        self.starts = (0, self.sizes[0], self.sizes[0] + self.sizes[1])
        self.total = sum(self.sizes)
        self.half = units(-(-self.total // 2)) * UNIT

    def source(self, t):
        a = t
        b = t - self.starts[1]
        c = t - self.starts[2]
        bv, bg = split_pow2(b, self.c3)
        cv, cg = split_pow2(c, self.c3)
        ck, cm = split_pow2(cv, self.grp)
        is_a = t < self.starts[1]
        is_b = t < self.starts[2]
        group = jnp.where(is_a, a, jnp.where(is_b, bg, cg))
        slot = jnp.where(is_a, 0, jnp.where(is_b, (bv + 1) * self.blk, cm * self.blk + ck + 1))
        local = jnp.where(is_a, a, jnp.where(is_b, b, c))
        count = jnp.where(is_a, self.counts[0], jnp.where(is_b, self.counts[1], self.counts[2]))
        return jnp.where(local < count, group * self.period, -(1 << 20)), slot


def flip(s, r):
    step = 1
    while step <= r:
        if r & step:
            s = s + step * (1 - 2 * ((s // step) % 2))
        step *= 2
    return s


def unfold(plan, x):
    x = x.astype(jnp.float32)
    low = pltpu.roll(x, HD, 1)[:plan.total - plan.half]
    return jnp.concatenate([x, low], axis=0).astype(jnp.bfloat16)


def kernel(
    plan, q_hbm, k_hbm, v_hbm, valid_hbm, offs_hbm, own_o, ret_r, back_hot,
    qkv_ref, valid_ref, offs_ref,
    buf_a, buf_b, buf_c, snd_a, snd_b, snd_c, snd_q, own_q, got_q, ret_s,
    load, zsend, zrecv, crecv, qsem, asend, afirst, arecv, bsend, brecv, fsend, frecv, rsem,
):
    G, B, N = plan.grp, plan.blk, plan.n
    R = plan.total
    K = G // 2
    H = plan.half
    gi, bi, si = lax.axis_index("grp"), lax.axis_index("blk"), lax.axis_index("set")
    core = gi % 2
    partner = gi + 1 - 2 * core
    even = si % 2 == 0

    def peer(sx, sy):
        return (lax.rem(gi + 2 * sx, G), lax.rem(bi + sy, B), si)


    load_offs = pltpu.make_async_copy(offs_hbm, offs_ref, load.at[0])
    load_valid = pltpu.make_async_copy(valid_hbm, valid_ref, load.at[1])
    load_qkv = [pltpu.make_async_copy(src, qkv_ref.at[n], load.at[2]) for n, src in enumerate((q_hbm, k_hbm, v_hbm))]
    for copy in (*load_qkv, load_offs, load_valid):
        copy.start()

    across = [(x, y) for x in range(K) for y in range(B) if x or y]
    near = [(x, y) for x, y in across if not (x and y)]
    diagonal = [(x, y) for x, y in across if x and y]

    barrier = pltpu.get_barrier_semaphore()

    def greet(device):
        pl.semaphore_signal(barrier, inc=1, device_id=device, device_id_type=MESH)

    for r in range(N - 1, 0, -1):
        greet((gi, bi, flip(si, r)))
    for x, y in near:
        greet(peer(x, y))
    greet((partner, bi, si))

    load_offs.wait()
    load_valid.wait()
    pltpu.make_async_copy(qkv_ref, qkv_ref, load.at[2]).wait()

    lane = lax.broadcasted_iota(jnp.int32, (R, LANES), 1)
    left = lane < HD
    base, slot = plan.source(lax.broadcasted_iota(jnp.int32, (R, plan.rows), 0))
    token = lax.broadcasted_iota(jnp.int32, (R, plan.rows), 1)
    valid_row = (valid_ref[...] > 0).astype(jnp.float32)
    flag_lane = lax.broadcasted_iota(jnp.int32, (UNIT, LANES), 1)

    moved = {}
    columns = {}
    for c in range(CHUNKS):
        cols = slice(c * LANES, (c + 1) * LANES)
        packed = jnp.concatenate([qkv_ref[n, :, cols] for n in range(3)], axis=1)
        hits = []
        for h in (2 * c, 2 * c + 1):
            hit = token == base + ((slot + offs_ref[1, h]) & (plan.period - 1))
            onehot = jnp.where(hit, jnp.float32(1), jnp.float32(0))
            columns[h] = jnp.sum(onehot * valid_row, axis=1, keepdims=True)
            hits.append(onehot.astype(jnp.bfloat16))
        both = jnp.dot(jnp.concatenate(hits, axis=0), packed, preferred_element_type=jnp.float32)
        moved[2 * c], moved[2 * c + 1] = both[:R], both[R:]

    def piece(h, which):
        return moved[h][:, which * LANES:(which + 1) * LANES]

    def fold(x, keep):
        low = x[H:]
        if R < 2 * H:
            low = jnp.concatenate([low, jnp.zeros((2 * H - R, LANES), low.dtype)], axis=0)
        return jnp.where(keep, x[:H], pltpu.roll(low, HD, 1))

    packs = []
    for number, (a, b, c) in enumerate(SETS):
        flags = jnp.zeros((UNIT, LANES), jnp.float32)
        for j, h in enumerate((a, b, c)):
            for u in range(R // UNIT):
                flags = jnp.where(
                    flag_lane == u * FLAG_STRIDE + j, columns[h][u * UNIT:(u + 1) * UNIT, :], flags
                )
        turned = pltpu.roll(piece(c, 2), HD, 1)
        mixed = jnp.where(left, piece(c, 1), turned) if number == 0 else jnp.where(left, turned, piece(c, 1))
        packs.append(
            (
                jnp.where(left, piece(a, 1), piece(b, 1)),
                jnp.where(left, piece(a, 2), piece(b, 2)),
                mixed,
                jnp.where(left, piece(a, 0), piece(b, 0)) * 0.125,
                piece(c, 0) * 0.125,
                flags,
                fold(piece(c, 0) * 0.125, left[:H] if number == 0 else ~left[:H]),
            )
        )
    mine = [jnp.where(even, x, y).astype(jnp.bfloat16) for x, y in zip(*packs)]
    other = [jnp.where(even, y, x).astype(jnp.bfloat16) for x, y in zip(*packs)]
    a_end, b_end = plan.starts[1], plan.starts[2]
    for j in range(PARTS):
        buf_a[0, 0, 0, j] = mine[j][:a_end]
        snd_a[j] = other[j][:a_end]
        buf_b[0, 0, j] = mine[j][a_end:b_end]
        snd_b[j] = other[j][a_end:b_end]
        buf_c[0, j] = mine[j][b_end:]
        snd_c[j] = other[j][b_end:]
    buf_a[0, 0, 0, PARTS, 0:UNIT] = mine[5]
    snd_a[PARTS, 0:UNIT] = other[5]
    for j in range(2):
        own_q[j] = mine[3 + j]
    snd_q[0:R] = other[3]
    snd_q[R:R + H] = other[6]

    pl.semaphore_wait(barrier, (N - 1) + len(near) + 1)

    heads = (slice(0, 2), slice(2, 3))
    line_sem = (lambda r: zrecv.at[0, r - 1], lambda r: zrecv.at[1, r - 1], lambda r: zrecv.at[2, r - 1])

    def line_ref(part, r):
        if part == 0:
            return buf_a.at[0, 0, r]
        if part < 3:
            return buf_b.at[0, r, heads[part - 1]]
        return buf_c.at[r, heads[part - 3]]

    def zcopy(part, r):
        sent = snd_a if part == 0 else (snd_b if part < 3 else snd_c).at[heads[(part - 1) % 2]]
        return pltpu.make_async_remote_copy(
            src_ref=sent if r % 2 else line_ref(part, 0),
            dst_ref=line_ref(part, r),
            send_sem=zsend.at[part],
            recv_sem=line_sem[part](r) if part < 3 else crecv.at[part - 3],
            device_id=(gi, bi, flip(si, r)), device_id_type=MESH,
        )

    def line_sent(part):
        rest = slice(1, N)
        ref = (
            buf_a.at[0, 0, rest] if part == 0
            else buf_b.at[0, rest, heads[part - 1]] if part < 3
            else buf_c.at[rest, heads[part - 3]]
        )
        pltpu.make_async_copy(ref, ref, zsend.at[part]).wait()

    def qcopy():
        return pltpu.make_async_remote_copy(
            src_ref=snd_q, dst_ref=got_q, send_sem=qsem.at[0], recv_sem=qsem.at[1],
            device_id=(gi, bi, flip(si, 1)), device_id_type=MESH,
        )

    def acopy(x, y, r):
        return pltpu.make_async_remote_copy(
            src_ref=buf_a.at[0, 0, r], dst_ref=buf_a.at[2 * x, y, r],
            send_sem=asend.at[x, y],
            recv_sem=afirst.at[y - 1] if x == 0 and r == 0 else arecv.at[x, y],
            device_id=peer((K - x) % K, (B - y) % B), device_id_type=MESH,
        )

    def bcopy(y, r, j):
        return pltpu.make_async_remote_copy(
            src_ref=buf_b.at[0, r, heads[j]], dst_ref=buf_b.at[y, r, heads[j]],
            send_sem=bsend.at[j, y - 1], recv_sem=brecv.at[j, y - 1],
            device_id=peer(0, B - y), device_id_type=MESH,
        )

    def fcopy(x, y):
        return pltpu.make_async_remote_copy(
            src_ref=buf_a.at[2 * x, y], dst_ref=buf_a.at[2 * x + 1, y],
            send_sem=fsend.at[x], recv_sem=frecv.at[x],
            device_id=(partner, bi, si), device_id_type=MESH,
        )

    def rcopy(j):
        rows = (slice(0, R), slice(R, R + H))[j]
        return pltpu.make_async_remote_copy(
            src_ref=ret_s.at[rows], dst_ref=ret_r.at[rows], send_sem=rsem.at[0, j], recv_sem=rsem.at[1, j],
            device_id=(gi, bi, flip(si, 1)), device_id_type=MESH,
        )

    def arrived(ref, sem):
        pltpu.make_async_copy(ref, ref, sem).wait()

    def spread_a(r, where):
        for x, y in where:
            acopy(x, y, r).start()

    def spread_b(r, j):
        for y in range(1, B):
            bcopy(y, r, j).start()

    order = list(range(N - 1, 0, -1))

    def send_line(part):
        for r in order:
            zcopy(part, r).start()

    send_line(0)
    spread_a(0, near)
    send_line(1)
    spread_b(0, 0)
    send_line(2)
    spread_b(0, 1)

    token = lax.broadcasted_iota(jnp.int32, (plan.rows, R), 0)
    base, slot = plan.source(lax.broadcasted_iota(jnp.int32, (plan.rows, R), 1))
    for h in range(HEAD_COUNT):
        hit = token == base + ((slot + offs_ref[1, h]) & (plan.period - 1))
        back_hot[h] = jnp.where(hit, jnp.float32(1), jnp.float32(0)).astype(jnp.bfloat16)

    for y in range(1, B):
        acopy(0, y, 0).wait_recv()
    spread_a(0, diagonal)
    for r in range(1, N):
        zcopy(0, r).wait_recv()
        spread_a(r, across)
    fcopy(0, 0).start()
    qcopy().start()
    send_line(3)
    send_line(4)
    for r in range(1, N):
        zcopy(1, r).wait_recv()
        spread_b(r, 0)
    for r in range(1, N):
        zcopy(2, r).wait_recv()
        spread_b(r, 1)
    for x, y in across:
        arrived(buf_a.at[2 * x, y] if x else buf_a.at[0, y, 1:N], arecv.at[x, y])
        fcopy(x, y).start()

    head_pick = lax.broadcasted_iota(jnp.int32, (FLAG_STRIDE, LANES), 1) & (FLAG_STRIDE - 1)
    head_pick = head_pick == lax.broadcasted_iota(jnp.int32, (FLAG_STRIDE, LANES), 0)
    head_pick = jnp.where(head_pick, jnp.float32(1), jnp.float32(0)).astype(jnp.bfloat16)

    def gather(level, at):
        pieces = []
        for u in range(plan.units[0]):
            rows = slice(u * UNIT, (u + 1) * UNIT)
            part = (buf_a[0, 0, :, at, rows], buf_a[0, :, :, at, rows], buf_a[:, :, :, at, rows])[level]
            pieces.append(part.reshape(-1, LANES))
        if level < 2:
            for u in range(plan.units[1]):
                rows = slice(u * UNIT, (u + 1) * UNIT)
                part = buf_b[0, :, at, rows] if level == 0 else buf_b[:, :, at, rows]
                pieces.append(part.reshape(-1, LANES))
        if level == 0:
            for u in range(plan.units[2]):
                pieces.append(buf_c[:, at, u * UNIT:(u + 1) * UNIT].reshape(-1, LANES))
        return pieces[0] if len(pieces) == 1 else jnp.concatenate(pieces, axis=0)

    def level_attend(level):
        M = (R, b_end, a_end)[level]
        tiles = M // UNIT
        devices = (N, B * N, G * B * N)[level]
        per_unit = devices * UNIT
        rows = slice(0, UNIT)
        at = PARTS
        tall = (buf_a[0, 0, :, at, rows], buf_a[0, :, :, at, rows], buf_a[:, :, :, at, rows])[level]
        tall = tall.reshape(per_unit, LANES).astype(jnp.float32)
        unit_lane = lax.broadcasted_iota(jnp.int32, (per_unit, LANES), 1) // FLAG_STRIDE
        tall = [jnp.where(unit_lane == u, tall, 0.0).astype(jnp.bfloat16) for u in range(tiles)]
        tall = tall[0] if tiles == 1 else jnp.concatenate(tall, axis=0)
        ok = lax.dot_general(
            head_pick, tall, (((1,), (1,)), ((), ())), preferred_element_type=jnp.float32
        )
        keys = per_unit * tiles
        diagonal_tile = lax.broadcasted_iota(jnp.int32, (UNIT, LANES), 1) - lax.broadcasted_iota(
            jnp.int32, (UNIT, LANES), 0
        )

        def allow(s, bias, who):
            masked = s + bias
            rows = []
            for u in range(tiles):
                at = slice(u * UNIT, (u + 1) * UNIT)
                spot = u * per_unit + who * UNIT
                tile = slice(spot // LANES * LANES, spot // LANES * LANES + LANES)
                fixed = jnp.where(diagonal_tile == spot % LANES, s[at, tile], masked[at, tile])
                pieces = [masked[at, :tile.start], fixed, masked[at, tile.stop:]]
                rows.append(jnp.concatenate([p for p in pieces if p.shape[1]], axis=1))
            return jnp.concatenate(rows, axis=0)

        bias = jnp.where(ok > 0.5, 0.0, NEG)
        half_lane = lax.broadcasted_iota(jnp.int32, (M, LANES), 1) < HD
        value_lane = half_lane != even
        contract = (((1,), (1,)), ((), ()))
        zero = jnp.zeros((M, LANES), jnp.bfloat16)

        def scores(part, who):
            q = own_q[part, 0:M] if who == 0 else got_q[0:M] if part == 0 else got_single[0:M]
            keys = gather(level, 2 * part)
            if part == 0:
                q = jnp.concatenate([jnp.where(half_lane, q, zero), jnp.where(half_lane, zero, q)], axis=0)
            else:
                q = jnp.where(value_lane, zero, q)
            s = lax.dot_general(q, keys, contract, preferred_element_type=jnp.float32)
            return [s[:M], s[M:]] if part == 0 else [s]

        def masked(s, part, who):
            return [allow(x, bias[2 * part + n:2 * part + n + 1, :], who) for n, x in enumerate(s)]

        def mix(probs, part):
            values = gather(level, 1 + part)
            return jnp.dot(jnp.concatenate(probs, axis=0), values, preferred_element_type=jnp.float32)

        def finish(mixed, tops, totals, part):
            if part == 1:
                return (mixed, *(jnp.broadcast_to(x[0], (M, LANES)) for x in (tops, totals)))
            return (
                jnp.where(half_lane, mixed[:M], mixed[M:]),
                *(jnp.where(half_lane, x[0], x[1]) for x in (tops, totals)),
            )

        return scores, masked, mix, finish

    def attend(jobs, who):
        scores = [level[0](part, who) for level, part in jobs]
        scores = [level[1](s, part, who) for s, (level, part) in zip(scores, jobs)]
        tops = [[jnp.max(x, axis=1, keepdims=True) for x in s] for s in scores]
        weights = [[jnp.exp(x - t) for x, t in zip(s, top)] for s, top in zip(scores, tops)]
        probs = [[x.astype(jnp.bfloat16) for x in w] for w in weights]
        mixed = [level[2](p, part) for p, (level, part) in zip(probs, jobs)]
        totals = [[jnp.sum(x, axis=1, keepdims=True) for x in w] for w in weights]
        return [
            level[3](m, top, total, part) for m, top, total, (level, part) in zip(mixed, tops, totals, jobs)
        ]

    def combine(*levels):
        highest = functools.reduce(jnp.maximum, [top for _, top, _ in levels])
        shares = [jnp.exp(top - highest) for _, top, _ in levels]
        return sum(s * m for s, (m, _, _) in zip(shares, levels)) / sum(
            s * total for s, (_, _, total) in zip(shares, levels)
        )

    qcopy().wait_recv()
    got_single = unfold(plan, got_q[R:R + H])
    middle, dense = level_attend(1), level_attend(0)
    for x in range(K):
        arrived(buf_a.at[2 * x + 1], frecv.at[x])
    outer = level_attend(2)
    value_half = left[:H] != even
    for who, j in ((1, 0), (1, 1), (0, 0), (0, 1)):
        if who == 1:
            for y in range(1, B):
                arrived(buf_b.at[y, :, heads[j]], brecv.at[j, y - 1])
            arrived(buf_c.at[1:N, heads[j]], crecv.at[j])
        jobs = [(middle, j), (dense, j)]
        if j == 0:
            second, first, *third = attend(jobs + [(outer, 0), (outer, 1)], who)
        else:
            second, first = attend(jobs, who)

        def rows(level, start, stop):
            return tuple(x[start:stop] for x in level)

        alone = rows(first, b_end, R)
        mixed = jnp.concatenate(
            [
                combine(rows(first, 0, a_end), rows(second, 0, a_end), third[j]),
                combine(rows(first, a_end, b_end), rows(second, a_end, b_end)),
                alone[0] / alone[2],
            ],
            axis=0,
        )
        if who == 0:
            own_o[j] = mixed.astype(jnp.bfloat16)
        else:
            if j == 0:
                ret_s[0:R] = mixed.astype(jnp.bfloat16)
            else:
                ret_s[R:R + H] = fold(mixed, value_half).astype(jnp.bfloat16)
            rcopy(j).start()
    for part in range(5):
        line_sent(part)
    qcopy().wait_send()
    for x, y in across:
        arrived(buf_a.at[0, 0], asend.at[x, y])
    for j in range(2):
        for y in range(1, B):
            arrived(buf_b.at[0, :, heads[j]], bsend.at[j, y - 1])
    for x in range(K):
        arrived(buf_a.at[2 * x], fsend.at[x])
    for j in range(2):
        rcopy(j).wait_recv()

    for j in range(2):
        rcopy(j).wait_send()


def project(plan, own_o, ret_r, back_hot, w_ref, o_ref):
    R, H = plan.total, plan.half
    even = lax.axis_index("set") % 2 == 0
    left = lax.broadcasted_iota(jnp.int32, (R, LANES), 1) < HD
    got = (ret_r[0:R], unfold(plan, ret_r[R:R + H]))
    sets = [
        (jnp.where(even, own_o[j], got[j]), jnp.where(even, got[j], own_o[j])) for j in range(2)
    ]
    (zero_pair, one_pair), (zero_single, one_single) = sets
    singles = jnp.where(left, one_single, zero_single)
    out_left = lax.broadcasted_iota(jnp.int32, (plan.rows, LANES), 1) < HD
    attention, weights = [], []
    for value, (a, b) in ((zero_pair, SETS[0][:2]), (one_pair, SETS[1][:2]), (singles, (SETS[1][2], SETS[0][2]))):
        back = [jnp.dot(back_hot[h], value, preferred_element_type=jnp.float32) for h in (a, b)]
        attention.append(jnp.where(out_left, back[0], back[1]).astype(jnp.bfloat16))
        weights += [w_ref[a * HD:(a + 1) * HD, :], w_ref[b * HD:(b + 1) * HD, :]]
    attention = jnp.concatenate(attention, axis=1)
    weights = jnp.concatenate(weights, axis=0)
    o_ref[...] = jnp.dot(attention, weights, preferred_element_type=jnp.float32).astype(o_ref.dtype)


def solution(mesh):
    G, B, N = mesh.shape["grp"], mesh.shape["blk"], mesh.shape["set"]

    def per_device(queries, keys, values, valid, offsets, w_out):
        rows, width = queries.shape
        plan = Plan(G, B, N, rows)
        vmem = pl.BlockSpec(memory_space=pltpu.VMEM)
        anywhere = pl.BlockSpec(memory_space=pl.ANY)
        dma = pltpu.SemaphoreType.DMA
        ra, rb, rc = plan.sizes
        R = plan.total
        bf16 = jnp.bfloat16
        outputs = ((2, R, LANES), (R + plan.half, LANES), (HEAD_COUNT, rows, R))
        attended = pl.pallas_call(
            functools.partial(kernel, plan),
            out_shape=[pltpu.VMEM(shape, bf16) for shape in outputs],
            in_specs=[anywhere] * 5,
            out_specs=[vmem] * 3,
            cost_estimate=pl.CostEstimate(
                flops=4 * rows * rows * N * width * 4, bytes_accessed=4 * rows * width * 2, transcendentals=0
            ),
            scratch_shapes=[
                pltpu.VMEM((3, rows, width), bf16),
                pltpu.VMEM((1, rows), jnp.int32),
                pltpu.SMEM(offsets.shape, jnp.int32),
                pltpu.VMEM((G, B, N, PARTS + 1, ra, LANES), bf16),
                pltpu.VMEM((B, N, PARTS, rb, LANES), bf16),
                pltpu.VMEM((N, PARTS, rc, LANES), bf16),
                pltpu.VMEM((PARTS + 1, ra, LANES), bf16),
                pltpu.VMEM((PARTS, rb, LANES), bf16),
                pltpu.VMEM((PARTS, rc, LANES), bf16),
                pltpu.VMEM((R + plan.half, LANES), bf16),
                pltpu.VMEM((2, R, LANES), bf16),
                pltpu.VMEM((R + plan.half, LANES), bf16),
                pltpu.VMEM((R + plan.half, LANES), bf16),
                dma((3,)),
                dma((5,)),
                dma((3, N - 1)),
                dma((2,)),
                dma((2,)),
                dma((G // 2, B)),
                dma((B - 1,)),
                dma((G // 2, B)),
                dma((2, B - 1)),
                dma((2, B - 1)),
                dma((G // 2,)),
                dma((G // 2,)),
                dma((2, 2)),
            ],
            compiler_params=pltpu.CompilerParams(
                collective_id=0, has_side_effects=True, vmem_limit_bytes=60 * 1024 * 1024
            ),
        )(queries, keys, values, valid.reshape(1, rows), offsets)
        return pl.pallas_call(
            functools.partial(project, plan),
            out_shape=jax.ShapeDtypeStruct((rows, w_out.shape[1]), bf16),
            in_specs=[vmem] * 4,
            out_specs=vmem,
            compiler_params=pltpu.CompilerParams(vmem_limit_bytes=8 * 1024 * 1024),
        )(*attended, w_out)

    rows_spec = P(("grp", "blk", "set"), None)
    return jax.shard_map(
        per_device,
        mesh=mesh,
        in_specs=(rows_spec, rows_spec, rows_spec, P(("grp", "blk", "set")), P(), P()),
        out_specs=rows_spec,
        check_vma=False,
    )
```
